32 devices in a mesh: real: 2 (over x), row: 16 (over z, y, core).
Axes of the slice: x: 2, y: 2, z: 4, core: 2. Of those that a mesh axis runs over, the one named last changes fastest.
Arguments:
- site_tensor: float32 [32, 2, 256, 256], P(('real', 'row')), parts along dimension 0, may hold values from -20 to 20
- left_env: float32 [32, 14, 256, 256], P(('real', 'row')), parts along dimension 0, may hold values from -10 to 10
- right_env: float32 [32, 14, 256, 256], P(('real', 'row')), parts along dimension 0, may hold values from -10 to 10
- sector_size: int32 [32], P('real'), parts along dimension 0, may hold values from 64 to 256
Outputs:
- left_out: float32 [32, 2, 256, 256], P(('real', 'row')), parts along dimension 0
- bond_out: float32 [32, 256, 256], P(('real', 'row')), parts along dimension 0
The draws below stay inside these ranges and needn't reach their ends.
There are 2 independent parts, one for each index of `real`. The reference program is written for one: setup_inputs(seed, part) draws one part's arguments, and reference() takes and returns one part's arrays. A program takes and returns all parts, laid end to end along the dimension named above; each array names one. Nothing has to cross between parts.
All inputs are finite; a program needn't handle non-finite values.
Results may differ from the reference program's by a relative error of at most 0.00005.
Values sent between devices are 32-bit elements; how exact they have to be, the bound alone decides.
No kernel may reach another device: no remote copies, remote signals or barrier semaphores. Data moves between devices by JAX's collectives and lax.ppermute only.
A program may use at most 64 MiB of HBM per device.

```python
import jax
import jax.numpy as jnp
from jax import lax

SEC = 256
W_DN = 4
W_UP = 4
W = 14
SECTORS = 16


def sector_ramp(total_rise):
    position = jnp.arange(SECTORS, dtype=jnp.float32) / max(SECTORS - 1, 1)
    return jnp.exp(jnp.log(total_rise) * position)


def draw_site_tensor(key, part):
    key_noise, key_scale = jax.random.split(jax.random.fold_in(key, 11))
    random_part = jnp.clip(jax.random.normal(key_noise, (SECTORS, 2, SEC, SEC), jnp.float32), -6.0, 6.0)
    column_scale = jnp.exp(jnp.clip(0.2 * jax.random.normal(key_scale, (SECTORS, 2, 1, SEC), jnp.float32), -0.8, 0.8))
    ramp = jnp.sqrt(sector_ramp(3.0))
    random_part = random_part * SEC ** (-0.5)
    identity = jnp.eye(SEC, dtype=jnp.float32)
    upper_block = identity[None] + 0.35 * random_part[:, 0]
    lower_block = 0.7 * random_part[:, 1]
    return jnp.stack([upper_block, lower_block], 1) * column_scale * ramp[:, None, None, None]


def environment_noise(key):
    noise = jnp.clip(jax.random.normal(key, (SECTORS, W, SEC, SEC), jnp.float32), -6.0, 6.0)
    return noise * SEC ** (-0.5)


def draw_left_env(key, part):
    key_noise, key_field = jax.random.split(jax.random.fold_in(key, 23))
    noise = environment_noise(key_noise)
    rough = jnp.exp(jax.random.uniform(key_field, (SECTORS, SEC), jnp.float32, jnp.log(0.5), jnp.log(2.0)))
    ramp = sector_ramp(3.0)
    field = rough * ramp[:, None]
    identity = jnp.eye(SEC, dtype=jnp.float32)
    onsite = field[:, :, None] * identity[None]
    return noise.at[:, W - 1].add(onsite)


def draw_right_env(key, part):
    noise = environment_noise(jax.random.fold_in(key, 37))
    identity = jnp.eye(SEC, dtype=jnp.float32)
    return noise.at[:, W - 1].add(identity[None])


def with_ends(values, own_key, least, high):
    dims = values.shape
    index_at = [jax.random.randint(jax.random.fold_in(own_key, axis), (), 0, dims[axis]) for axis in range(len(dims))]
    values = values.at[tuple(index_at)].set(least)
    longest = dims.index(max(dims))
    index_at[longest] = (index_at[longest] + 1) % dims[longest]
    return values.at[tuple(index_at)].set(high)


def setup_inputs(seed: int = 0, part: int = 0) -> dict:
    seeds = jax.random.split(jax.random.key(seed), 5)
    part_keys = jax.random.split(jax.random.fold_in(seeds[4], part), 5)
    site_tensor = draw_site_tensor(jax.random.fold_in(jax.random.fold_in(seeds[4], part), 71), part)
    left_env = draw_left_env(jax.random.fold_in(jax.random.fold_in(seeds[4], part), 71), part)
    right_env = draw_right_env(jax.random.fold_in(jax.random.fold_in(seeds[4], part), 71), part)
    sector_size = with_ends(jax.random.randint(part_keys[3], (SECTORS,), SEC // 4, SEC + 1), jax.random.fold_in(part_keys[3], 1), SEC // 4, SEC).astype(jnp.int32)
    return {"site_tensor": site_tensor, "left_env": left_env, "right_env": right_env, "sector_size": sector_size}


highest = lax.Precision.HIGHEST
time_step = 0.15

def solve_rows(factor, stacked):
    return jax.scipy.linalg.solve_triangular(factor, stacked.T, lower=True).T

def apply_bond(operand, left_env, right_env, mask_pair):
    products = jnp.einsum('sik,sakl->sail', operand, right_env, precision=highest)
    empty_block = jnp.zeros_like(products[:1])
    down_terms = jnp.concatenate([empty_block[:, :W_DN], products[:-1, :W_DN]], 0)
    upper_terms = jnp.concatenate([products[1:, W_DN:W_DN + W_UP], empty_block[:, W_DN:W_DN + W_UP]], 0)
    combined = jnp.concatenate([down_terms, upper_terms, products[:, W_DN + W_UP:]], 1)
    return jnp.einsum('saij,sajl->sil', left_env, combined, precision=highest) * mask_pair

def reference(site_tensor, left_env, right_env, sector_size):
    live_mask = (jnp.arange(SEC, dtype=jnp.int32)[None, :] < sector_size[:, None]).astype(jnp.float32)
    row_mask = live_mask[:, :, None]
    col_mask = live_mask[:, None, :]
    mask_pair = row_mask * col_mask
    upper_block = site_tensor[:, 0] * mask_pair
    lower_source = site_tensor[:, 1] * row_mask
    lower_block = jnp.concatenate([jnp.zeros_like(lower_source[:1]), lower_source[:-1]], 0) * col_mask
    stacked = jnp.concatenate([upper_block, lower_block], 1)
    identity = jnp.eye(SEC, dtype=jnp.float32)
    gram_matrix = jnp.einsum('sij,sik->sjk', stacked, stacked, precision=highest) + identity[None] * (1.0 - live_mask)[:, None, :]
    factor = jnp.linalg.cholesky(gram_matrix)
    orthonormal = jax.vmap(solve_rows)(factor, stacked)
    moved_back = jnp.concatenate([orthonormal[1:, SEC:], jnp.zeros_like(orthonormal[:1, SEC:])], 0)
    left_out = jnp.stack([orthonormal[:, :SEC], moved_back], 1)
    bond_matrix = jnp.swapaxes(factor, 1, 2) * mask_pair
    start_norm = jnp.sum(bond_matrix * bond_matrix)
    applied = apply_bond(bond_matrix, left_env, right_env, mask_pair)
    energy = jnp.sum(bond_matrix * applied) / start_norm
    shifted = applied - energy * bond_matrix
    second = apply_bond(shifted, left_env, right_env, mask_pair) - energy * shifted
    evolved = bond_matrix + time_step * shifted + 0.5 * time_step * time_step * second
    final_norm = jnp.sum(evolved * evolved)
    return (left_out, evolved * jnp.sqrt(start_norm / final_norm))
```

```python
import jax
import jax.numpy as jnp
from jax import lax
from jax.sharding import PartitionSpec as P

W_DN = 4
W_UP = 4


highest = lax.Precision.HIGHEST
high = lax.Precision.HIGH
time_step = 0.15


def shifted_2(value, axis, steps):
    count = lax.axis_size(axis)
    leading, last = (max(0, -steps), min(count, count - steps))
    return lax.ppermute(value, axis, [(source, source + steps) for source in range(leading, last)])


def row_sum(partials):
    count = lax.axis_size("row")
    spread = jnp.broadcast_to(partials[None], (count,) + partials.shape)
    return jnp.sum(lax.all_to_all(spread, "row", 0, 0, tiled=True), 0)


def apply_moved(operand, left_local, right_local, right_down, right_upper, mask_pair):
    low = shifted_2(operand, "row", 1)
    upper = shifted_2(operand, "row", -1)
    own_terms = jnp.einsum("ik,akl->ail", operand, right_local[W_DN + W_UP :], precision=high)
    own = jnp.einsum("aij,ajl->il", left_local[W_DN + W_UP :], own_terms, precision=high)
    down_terms = jnp.einsum("ik,akl->ail", low, right_down, precision=high)
    upper_terms = jnp.einsum("ik,akl->ail", upper, right_upper, precision=high)
    moved = jnp.einsum("aij,ajl->il", left_local[:W_DN], down_terms, precision=high)
    moved += jnp.einsum("aij,ajl->il", left_local[W_DN : W_DN + W_UP], upper_terms, precision=high)
    return (own + moved) * mask_pair


def on_device(site_tensor, left_env, right_env, sector_size):
    states = site_tensor.shape[-1]
    left_local = left_env[0]
    right_local = right_env[0]
    own_size = lax.dynamic_index_in_dim(sector_size, lax.axis_index("row"), 0, keepdims=False)
    live_mask = (jnp.arange(states, dtype=jnp.int32) < own_size).astype(jnp.float32)
    mask_pair = live_mask[:, None] * live_mask[None, :]
    lower_source = site_tensor[0, 1] * live_mask[:, None]
    lower_block = shifted_2(lower_source, "row", 1) * live_mask[None, :]
    right_down = shifted_2(right_local[:W_DN], "row", 1)
    right_upper = shifted_2(right_local[W_DN : W_DN + W_UP], "row", -1)
    upper_block = site_tensor[0, 0] * mask_pair
    stacked = jnp.concatenate([upper_block, lower_block], 0)
    identity = jnp.eye(states, dtype=jnp.float32)
    gram_matrix = (
        jnp.einsum("ij,ik->jk", stacked, stacked, precision=highest)
        + identity * (1.0 - live_mask)[None, :]
    )
    factor = jnp.linalg.cholesky(gram_matrix)
    bond_matrix = factor.T * mask_pair

    def operator(operand):
        return apply_moved(operand, left_local, right_local, right_down, right_upper, mask_pair)

    orthonormal = jax.scipy.linalg.solve_triangular(factor, stacked.T, lower=True).T
    moved_back = shifted_2(orthonormal[states:], "row", -1)
    left_out = jnp.stack([orthonormal[:states], moved_back], 0)[None]

    applied = operator(bond_matrix)
    lanes = jnp.arange(128)[None]
    norm_row = jnp.where(lanes == 0, jnp.sum(bond_matrix * bond_matrix), 0.0)
    local_row = jnp.where(lanes == 1, jnp.sum(bond_matrix * applied), norm_row)
    sums = row_sum(local_row)
    start_norm = sums[0, 0]
    energy = sums[0, 1] / start_norm
    twice = operator(applied)
    shifted = applied - energy * bond_matrix
    second = twice - energy * applied - energy * shifted
    evolved = bond_matrix + time_step * shifted + 0.5 * time_step * time_step * second
    final_row = jnp.where(lanes == 0, jnp.sum(evolved * evolved), 0.0)
    final_norm = row_sum(final_row)[0, 0]
    return (left_out, (evolved * jnp.sqrt(start_norm / final_norm))[None])


def solution(mesh):
    placed = (
        P(("real", "row"), None, None, None),
        P(("real", "row"), None, None, None),
        P(("real", "row"), None, None, None),
        P("real"),
    )
    return jax.shard_map(
        on_device,
        mesh=mesh,
        in_specs=placed,
        out_specs=(P(("real", "row"), None, None, None), P(("real", "row"), None, None)),
        check_vma=False,
    )
```

```python
import functools

import jax
import jax.numpy as jnp
from jax import lax
from jax.experimental import pallas as pl
from jax.experimental.pallas import tpu as pltpu
from jax.sharding import PartitionSpec as P

W_DN = 4
W_UP = 4
PANEL = 16
LANES = 128

f32, bf16 = jnp.float32, jnp.bfloat16
time_step = 0.15

VM = pl.BlockSpec(memory_space=pltpu.VMEM)
SM = pl.BlockSpec(memory_space=pltpu.SMEM)
ANY = pl.BlockSpec(memory_space=pl.ANY)
HB = pl.BlockSpec(memory_space=pltpu.HBM)


def params(mib):
    return pltpu.CompilerParams(vmem_limit_bytes=mib << 20)


def split2(x):
    hi = x.astype(bf16)
    return hi, (x - hi.astype(f32)).astype(bf16)


def split3(x):
    hi = x.astype(bf16)
    rest = x - hi.astype(f32)
    mid = rest.astype(bf16)
    return hi, mid, (rest - mid.astype(f32)).astype(bf16)


def dot(a, b, ca=1, cb=0):
    return lax.dot_general(a, b, (((ca,), (cb,)), ((), ())), preferred_element_type=f32)


def dot3(a, b):
    ah, al = a
    bh, bl = b
    return dot(ah, bh) + dot(al, bh) + dot(ah, bl)


def dot6(a, b, cb=0):
    ah, am, al = a
    bh, bm, bl = b
    pairs = ((ah, bh), (ah, bm), (am, bh), (am, bm), (ah, bl), (al, bh))
    return sum(dot(x, y, 1, cb) for x, y in pairs)


def places(n, rows=None):
    shape = (n if rows is None else rows, n)
    return lax.broadcasted_iota(jnp.int32, shape, 0), lax.broadcasted_iota(jnp.int32, shape, 1)


def own_sizes(sizes):
    q = lax.axis_index("row")
    return q, sizes[q], sizes[jnp.maximum(q - 1, 0)]


def pick_kernel(right, after, out, sem, *, far):
    odd = lax.rem(lax.axis_index("row"), 2)
    first = (1 - odd if far else odd) * W_DN
    copy = pltpu.make_async_copy(right.at[0, pl.ds(first, W_UP)], out, sem.at[0])
    copy.start()
    copy.wait()


def pick(right, after, far):
    n = right.shape[-1]
    return pl.pallas_call(
        functools.partial(pick_kernel, far=far),
        out_shape=jax.ShapeDtypeStruct((W_UP, n, n), f32),
        in_specs=[HB, ANY],
        out_specs=ANY,
        scratch_shapes=[pltpu.SemaphoreType.DMA((1,))],
        compiler_params=params(4),
        name="pick",
    )(pltpu.with_memory_space_constraint(right, pltpu.HBM), after)


def factor_kernel(sizes, site, lower, bond, inv0, packed, work, turn, rows, erows, lstack, rstack):
    n = lower.shape[-1]
    _, own, prev = own_sizes(sizes)
    row_id, col_id = places(n)
    live_col = col_id < own
    top = jnp.where(live_col & (row_id < own), site[0, 0], 0.0)
    bot = jnp.where(live_col & (row_id < prev), lower[...], 0.0)
    gram = jnp.where((row_id == col_id) & (row_id >= own), 1.0, 0.0)
    for part in (top, bot):
        gram = gram + dot6(split3(part.T), split3(part))
    work[pl.ds(0, n), :] = gram
    work[pl.ds(n, PANEL), :] = jnp.zeros((PANEL, n), f32)
    lstack[...] = jnp.zeros(lstack.shape, bf16)
    rstack[...] = jnp.zeros(rstack.shape, bf16)
    inv0[...] = jnp.zeros((n, n), f32)
    lane = lax.broadcasted_iota(jnp.int32, (PANEL, LANES), 1)
    sub = lax.broadcasted_iota(jnp.int32, (PANEL, LANES), 0)
    tiles = n // LANES

    def body(p, carry):
        r0 = pl.multiple_of(p * PANEL, PANEL)
        tile = pl.multiple_of((r0 // LANES) * LANES, LANES)
        off = r0 - tile
        after = r0 + PANEL
        ntile = pl.multiple_of(jnp.minimum((after // LANES) * LANES, n - LANES), LANES)
        noff = pl.multiple_of(lax.rem(after, LANES), PANEL)
        w = work[pl.ds(r0, PANEL), :]
        diag = work[pl.ds(r0, PANEL), pl.ds(tile, LANES)]
        turn[...] = work[pl.ds(r0, PANEL), pl.ds(ntile, LANES)].T
        update = dot(lstack[...], rstack[...], 0, 0)
        ahead = turn[pl.ds(noff, PANEL), :]
        here, there = [], []
        for j in range(PANEL):
            at = jnp.full((PANEL, LANES), off + j, jnp.int32)
            here.append(jnp.take_along_axis(diag, at, axis=1, mode="promise_in_bounds"))
            there.append(jnp.broadcast_to(ahead[:, j : j + 1], (PANEL, LANES)))
        ext = jnp.where(lane == off + sub, 1.0, 0.0)
        acc = jnp.zeros((PANEL, n), f32)
        for k in range(PANEL):
            scale = lax.rsqrt(jnp.broadcast_to(here[k][k : k + 1, :], (PANEL, LANES)))
            a = here[k] * scale
            b = there[k] * scale
            rk = w[k : k + 1, :] * jnp.concatenate([scale[:1]] * tiles, 1)
            ek = ext[k : k + 1, :] * scale[:1]
            rows[k : k + 1, :] = rk
            erows[k : k + 1, :] = ek
            spread = jnp.broadcast_to(rk, (PANEL, n))
            acc = acc + jnp.concatenate([b] * tiles, 1) * spread
            if k + 1 < PANEL:
                w = w - jnp.concatenate([a] * tiles, 1) * spread
                ext = ext - a * jnp.broadcast_to(ek, (PANEL, LANES))
            for j in range(k + 1, PANEL):
                s = jnp.broadcast_to(a[j : j + 1, :], (PANEL, LANES))
                here[j] = here[j] - a * s
                there[j] = there[j] - b * s
        work[pl.ds(0, n), :] = work[pl.ds(0, n), :] - update
        work[pl.ds(after, PANEL), :] = work[pl.ds(after, PANEL), :] - acc
        r = rows[...]
        inv0[pl.ds(r0, PANEL), pl.ds(tile, LANES)] = erows[...]
        h, m, l = split3(r)
        for i, (x, y) in enumerate(((h, h), (m, h), (h, m), (m, m), (l, h), (h, l))):
            lstack[pl.ds(i * PANEL, PANEL), :] = x
            rstack[pl.ds(i * PANEL, PANEL), :] = y
        rid, cid = places(n, PANEL)
        rid = rid + r0
        bond[pl.ds(r0, PANEL), :] = jnp.where((cid >= rid) & (rid < own) & (cid < own), r, 0.0)
        return carry

    lax.fori_loop(0, n // PANEL, body, 0)
    at = 0
    for i in range(tiles):
        for j in range(i, tiles):
            packed[pl.ds(at, LANES), :] = bond[pl.ds(i * LANES, LANES), pl.ds(j * LANES, LANES)]
            at += LANES


def factor(sizes, site, lower):
    n = lower.shape[-1]
    tiles = n // LANES
    return pl.pallas_call(
        factor_kernel,
        out_shape=[jax.ShapeDtypeStruct((n, n), f32)] * 2
        + [jax.ShapeDtypeStruct((tiles * (tiles + 1) // 2 * LANES, LANES), f32)],
        in_specs=[SM, VM, VM],
        out_specs=[VM] * 3,
        scratch_shapes=[
            pltpu.VMEM((n + PANEL, n), f32),
            pltpu.VMEM((LANES, PANEL), f32),
            pltpu.VMEM((PANEL, n), f32),
            pltpu.VMEM((PANEL, LANES), f32),
            pltpu.VMEM((6 * PANEL, n), bf16),
            pltpu.VMEM((6 * PANEL, n), bf16),
        ],
        compiler_params=params(12),
        name="factor",
    )(sizes, site, lower)


def inverse_kernel(bond, inv0, out):
    n = bond.shape[-1]
    rid, cid = places(n)
    low_tri = bond[...].T
    x = inv0[...]
    size = PANEL
    while size < n:
        off = (rid // (2 * size) == cid // (2 * size)) & (rid // size > cid // size)
        part = split3(jnp.where(off, low_tri, 0.0))
        xs = split3(x)
        x = x - dot6(xs, split3(dot6(part, xs)))
        size *= 2
    out[...] = x


def inverse(bond, inv0):
    n = bond.shape[-1]
    return pl.pallas_call(
        inverse_kernel,
        out_shape=jax.ShapeDtypeStruct((n, n), f32),
        in_specs=[VM] * 2,
        out_specs=VM,
        compiler_params=params(16),
        name="inverse",
    )(bond, inv0)


def ortho_kernel(sizes, inv, site, lower, top_out, low_out):
    n = inv.shape[-1]
    _, own, prev = own_sizes(sizes)
    rid, cid = places(n)
    xs = split3(inv[...])
    live_col = cid < own
    low_out[...] = dot6(split3(jnp.where(live_col & (rid < prev), lower[...], 0.0)), xs, 1)
    top_out[...] = dot6(split3(jnp.where(live_col & (rid < own), site[0, 0], 0.0)), xs, 1)


def ortho(sizes, inv, site, lower):
    n = inv.shape[-1]
    return pl.pallas_call(
        ortho_kernel,
        out_shape=[jax.ShapeDtypeStruct((n, n), f32)] * 2,
        in_specs=[SM] + [VM] * 3,
        out_specs=[VM] * 2,
        compiler_params=params(16),
        name="ortho",
    )(sizes, inv, site, lower)


def channel(left, a, field, right):
    return dot3(split2(left[0, a]), split2(dot3(field, split2(right))))


def own_kernel(field, left, right, out):
    f = split2(field[...])
    total = None
    for a in range(W_DN + W_UP, left.shape[1]):
        term = channel(left, a, f, right[0, a])
        total = term if total is None else total + term
    out[...] = total


def own_terms(field, left, right):
    n = field.shape[-1]
    return pl.pallas_call(
        own_kernel,
        out_shape=jax.ShapeDtypeStruct((n, n), f32),
        in_specs=[VM] * 3,
        out_specs=VM,
        compiler_params=params(16),
        name="own",
    )(field, left, right)


def unpacked(ref, n):
    if ref.shape[-1] == n:
        return ref[...]
    tiles, at, rows = n // LANES, 0, []
    for i in range(tiles):
        row = [jnp.zeros((LANES, LANES), f32)] * i
        for _ in range(i, tiles):
            row.append(ref[pl.ds(at, LANES), :])
            at += LANES
        rows.append(jnp.concatenate(row, 1))
    return jnp.concatenate(rows, 0)


def moved_total(near, far, left, right_near, right_far, part, own):
    odd = lax.rem(lax.axis_index("row"), 2)
    total = part[...]
    for field, right, base in ((near, right_near, (1 - odd) * W_DN), (far, right_far, odd * W_DN)):
        f = split2(unpacked(field, part.shape[-1]))
        for a in range(right.shape[0]):
            total = total + channel(left, base + a, f, right[a])
    rid, cid = places(part.shape[-1])
    return jnp.where((rid < own) & (cid < own), total, 0.0)


def first_kernel(sizes, near, far, left, right_near, right_far, part, out):
    _, own, _ = own_sizes(sizes)
    out[...] = moved_total(near, far, left, right_near, right_far, part, own)


def first_apply(sizes, near, far, left, right_near, right_far, part):
    n = part.shape[-1]
    return pl.pallas_call(
        first_kernel,
        out_shape=jax.ShapeDtypeStruct((n, n), f32),
        in_specs=[SM] + [VM] * 6,
        out_specs=VM,
        compiler_params=params(16),
        name="first",
    )(sizes, near, far, left, right_near, right_far, part)


def second_kernel(sizes, near, far, left, right_near, right_far, part, bond, applied, out, spread):
    _, own, _ = own_sizes(sizes)
    twice = moved_total(near, far, left, right_near, right_far, part, own)
    out[...] = twice
    basis = (bond[...], time_step * applied[...], (0.5 * time_step * time_step) * twice)
    sums = []
    for i in range(3):
        for j in range(i, 3):
            line = jnp.sum(basis[i] * basis[j], 0, keepdims=True)
            sums.append(sum(line[:, t : t + LANES] for t in range(0, line.shape[1], LANES)))
    block = jnp.concatenate(sums + [jnp.zeros((2, LANES), f32)], 0)
    for i in range(spread.shape[0]):
        spread[i] = block


def second_apply(sizes, near, far, left, right_near, right_far, part, bond, applied, count):
    n = part.shape[-1]
    return pl.pallas_call(
        second_kernel,
        out_shape=[
            jax.ShapeDtypeStruct((n, n), f32),
            jax.ShapeDtypeStruct((count, 8, LANES), f32),
        ],
        in_specs=[SM] + [VM] * 8,
        out_specs=[VM, VM],
        compiler_params=params(16),
        name="second",
    )(sizes, near, far, left, right_near, right_far, part, bond, applied)


def stack_kernel(top, back, out, sems):
    top_copy = pltpu.make_async_copy(top, out.at[0, 0], sems.at[0])
    back_copy = pltpu.make_async_copy(back, out.at[0, 1], sems.at[1])
    top_copy.start()
    back_copy.start()
    top_copy.wait()
    back_copy.wait()


def stack(top, back):
    n = top.shape[-1]
    return pl.pallas_call(
        stack_kernel,
        out_shape=jax.ShapeDtypeStruct((1, 2, n, n), f32),
        in_specs=[ANY] * 2,
        out_specs=ANY,
        scratch_shapes=[pltpu.SemaphoreType.DMA((2,))],
        compiler_params=params(4),
        name="stack",
    )(top, back)


def final_kernel(gathered, bond, applied, twice, out):
    sums = jnp.sum(jnp.sum(gathered[...], 0), 1, keepdims=True)
    bb, ba, bt, aa, at, tt = (jnp.broadcast_to(sums[i : i + 1, :], (1, bond.shape[-1])) for i in range(6))
    rate = ba / bb
    c0 = 1.0 - rate + 0.5 * rate * rate
    c1 = 1.0 - rate
    norm = c0 * (c0 * bb + 2.0 * (c1 * ba + bt)) + c1 * (c1 * aa + 2.0 * at) + tt
    scale = jnp.sqrt(bb / norm)
    steps = (c0 * scale, (c1 * time_step) * scale, (0.5 * time_step * time_step) * scale)
    out[0] = steps[0] * bond[...] + steps[1] * applied[...] + steps[2] * twice[...]


def final(gathered, bond, applied, twice):
    n = bond.shape[-1]
    return pl.pallas_call(
        final_kernel,
        out_shape=jax.ShapeDtypeStruct((1, n, n), f32),
        in_specs=[VM] * 4,
        out_specs=VM,
        compiler_params=params(4),
        name="final",
    )(gathered, bond, applied, twice)


def shifted_by(value, steps):
    count = lax.axis_size("row")
    first, last = max(0, -steps), min(count, count - steps)
    return lax.ppermute(value, "row", [(source, source + steps) for source in range(first, last)])


def swapped(value, first):
    count = lax.axis_size("row")
    pairs = [(i, i + 1) for i in range(first, count - 1, 2)]
    return lax.ppermute(value, "row", pairs + [(j, i) for i, j in pairs])


def bond_update(site, left, right, sizes):
    count = lax.axis_size("row")
    source = site[0, 1]
    lower = shifted_by(source, 1)
    to_far = pick(right, source, True)
    right_far = swapped(to_far, 1)
    to_near = pick(right, source, False)
    right_near = swapped(to_near, 0)
    bond, inv0, packed = factor(sizes, site, lower)
    far = swapped(packed, 1)
    near = swapped(packed, 0)
    part = own_terms(bond, left, right)
    inv = inverse(bond, inv0)
    applied = first_apply(sizes, near, far, left, right_near, right_far, part)
    far = swapped(applied, 1)
    near = swapped(applied, 0)
    part = own_terms(applied, left, right)
    top, low = ortho(sizes, inv, site, lower)
    back = shifted_by(low, -1)
    twice, spread = second_apply(sizes, near, far, left, right_near, right_far, part, bond, applied, count)
    gathered = lax.all_to_all(spread, "row", 0, 0, tiled=True)
    left_out = stack(top, back)
    bond_out = final(gathered, bond, applied, twice)
    return left_out, bond_out


def solution(mesh):
    placed = (
        P(("real", "row"), None, None, None),
        P(("real", "row"), None, None, None),
        P(("real", "row"), None, None, None),
        P("real"),
    )
    return jax.shard_map(
        bond_update,
        mesh=mesh,
        in_specs=placed,
        out_specs=(P(("real", "row"), None, None, None), P(("real", "row"), None, None)),
        check_vma=False,
    )
```

```python
import jax
import jax.numpy as jnp
from jax import lax
from jax.experimental import pallas as pl
from jax.experimental.pallas import tpu as pltpu
from jax.sharding import PartitionSpec as P

W_DN = 4
W_UP = 4
PANEL = 16
LANES = 128

f32, bf16 = jnp.float32, jnp.bfloat16
time_step = 0.15

VM = pl.BlockSpec(memory_space=pltpu.VMEM)
SM = pl.BlockSpec(memory_space=pltpu.SMEM)
ANY = pl.BlockSpec(memory_space=pl.ANY)
HB = pl.BlockSpec(memory_space=pltpu.HBM)


def params(mib):
    return pltpu.CompilerParams(vmem_limit_bytes=mib << 20)


def split2(x):
    hi = x.astype(bf16)
    return hi, (x - hi.astype(f32)).astype(bf16)


def split3(x):
    hi = x.astype(bf16)
    rest = x - hi.astype(f32)
    mid = rest.astype(bf16)
    return hi, mid, (rest - mid.astype(f32)).astype(bf16)


def dot(a, b, ca=1, cb=0):
    return lax.dot_general(a, b, (((ca,), (cb,)), ((), ())), preferred_element_type=f32)


def dot3(a, b):
    ah, al = a
    bh, bl = b
    return dot(ah, bh) + dot(al, bh) + dot(ah, bl)


def dot6(a, b, cb=0):
    ah, am, al = a
    bh, bm, bl = b
    pairs = ((ah, bh), (ah, bm), (am, bh), (am, bm), (ah, bl), (al, bh))
    return sum(dot(x, y, 1, cb) for x, y in pairs)


def places(n, rows=None):
    shape = (n if rows is None else rows, n)
    return lax.broadcasted_iota(jnp.int32, shape, 0), lax.broadcasted_iota(jnp.int32, shape, 1)


def own_sizes(sizes):
    q = lax.axis_index("row")
    return q, sizes[q], sizes[jnp.maximum(q - 1, 0)]


def far_kind(q):
    return lax.rem((q + 1) // 2, 2)


def take_far_kernel(site, right, source, early, middle, late, sems):
    q = lax.axis_index("row")
    half = W_UP // 2
    first = (1 - lax.rem(q, 2)) * W_DN
    turn = jnp.where(far_kind(q) == 0, first + half, first)
    copies = [pltpu.make_async_copy(site.at[0, 1], source, sems.at[0])]
    for i, (start, out) in enumerate(((first, early), (turn, middle), (first + half, late))):
        copies.append(pltpu.make_async_copy(right.at[0, pl.ds(start, half)], out, sems.at[i + 1]))
    for copy in copies:
        copy.start()
    for copy in copies:
        copy.wait()


def in_hbm(x):
    return pltpu.with_memory_space_constraint(x, pltpu.HBM)


def take_far(site, right):
    n = right.shape[-1]
    return pl.pallas_call(
        take_far_kernel,
        out_shape=[jax.ShapeDtypeStruct((n, n), f32)] + [jax.ShapeDtypeStruct((W_UP // 2, n, n), f32)] * 3,
        in_specs=[HB] * 2,
        out_specs=[ANY] * 4,
        scratch_shapes=[pltpu.SemaphoreType.DMA((4,))],
        compiler_params=params(4),
        name="take_far",
    )(in_hbm(site), in_hbm(right))


def take_near_kernel(right, near, sem):
    odd = lax.rem(lax.axis_index("row"), 2)
    copy = pltpu.make_async_copy(right.at[0, pl.ds(odd * W_DN, W_DN)], near, sem.at[0])
    copy.start()
    copy.wait()


def take_near(right):
    n = right.shape[-1]
    return pl.pallas_call(
        take_near_kernel,
        out_shape=jax.ShapeDtypeStruct((W_DN, n, n), f32),
        in_specs=[HB],
        out_specs=ANY,
        scratch_shapes=[pltpu.SemaphoreType.DMA((1,))],
        compiler_params=params(4),
        name="take_near",
    )(in_hbm(right))


def factor_kernel(sizes, site, lower, bond, packed, inv0, work, turn, rows, erows, lstack, rstack):
    n = lower.shape[-1]
    _, own, prev = own_sizes(sizes)
    row_id, col_id = places(n)
    live_col = col_id < own
    top = jnp.where(live_col & (row_id < own), site[0, 0], 0.0)
    bot = jnp.where(live_col & (row_id < prev), lower[...], 0.0)
    gram = jnp.where((row_id == col_id) & (row_id >= own), 1.0, 0.0)
    for part in (top, bot):
        gram = gram + dot6(split3(part.T), split3(part))
    work[pl.ds(0, n), :] = gram
    work[pl.ds(n, PANEL), :] = jnp.zeros((PANEL, n), f32)
    lstack[...] = jnp.zeros(lstack.shape, bf16)
    rstack[...] = jnp.zeros(rstack.shape, bf16)
    inv0[...] = jnp.zeros((n, n), f32)
    lane = lax.broadcasted_iota(jnp.int32, (PANEL, LANES), 1)
    sub = lax.broadcasted_iota(jnp.int32, (PANEL, LANES), 0)
    tiles = n // LANES

    def body(p, carry):
        r0 = pl.multiple_of(p * PANEL, PANEL)
        tile = pl.multiple_of((r0 // LANES) * LANES, LANES)
        off = r0 - tile
        after = r0 + PANEL
        ntile = pl.multiple_of(jnp.minimum((after // LANES) * LANES, n - LANES), LANES)
        noff = pl.multiple_of(lax.rem(after, LANES), PANEL)
        w = work[pl.ds(r0, PANEL), :]
        diag = work[pl.ds(r0, PANEL), pl.ds(tile, LANES)]
        turn[...] = work[pl.ds(r0, PANEL), pl.ds(ntile, LANES)].T
        update = dot(lstack[...], rstack[...], 0, 0)
        ahead = turn[pl.ds(noff, PANEL), :]
        here, there = [], []
        for j in range(PANEL):
            at = jnp.full((PANEL, LANES), off + j, jnp.int32)
            here.append(jnp.take_along_axis(diag, at, axis=1, mode="promise_in_bounds"))
            there.append(jnp.broadcast_to(ahead[:, j : j + 1], (PANEL, LANES)))
        ext = jnp.where(lane == off + sub, 1.0, 0.0)
        acc = jnp.zeros((PANEL, n), f32)
        for k in range(PANEL):
            scale = lax.rsqrt(jnp.broadcast_to(here[k][k : k + 1, :], (PANEL, LANES)))
            a = here[k] * scale
            b = there[k] * scale
            rk = w[k : k + 1, :] * jnp.concatenate([scale[:1]] * tiles, 1)
            ek = ext[k : k + 1, :] * scale[:1]
            rows[k : k + 1, :] = rk
            erows[k : k + 1, :] = ek
            spread = jnp.broadcast_to(rk, (PANEL, n))
            acc = acc + jnp.concatenate([b] * tiles, 1) * spread
            if k + 1 < PANEL:
                w = w - jnp.concatenate([a] * tiles, 1) * spread
                ext = ext - a * jnp.broadcast_to(ek, (PANEL, LANES))
            for j in range(k + 1, PANEL):
                s = jnp.broadcast_to(a[j : j + 1, :], (PANEL, LANES))
                here[j] = here[j] - a * s
                there[j] = there[j] - b * s
        work[pl.ds(0, n), :] = work[pl.ds(0, n), :] - update
        work[pl.ds(after, PANEL), :] = work[pl.ds(after, PANEL), :] - acc
        r = rows[...]
        inv0[pl.ds(r0, PANEL), pl.ds(tile, LANES)] = erows[...]
        h, m, l = split3(r)
        for i, (x, y) in enumerate(((h, h), (m, h), (h, m), (m, m), (l, h), (h, l))):
            lstack[pl.ds(i * PANEL, PANEL), :] = x
            rstack[pl.ds(i * PANEL, PANEL), :] = y
        rid, cid = places(n, PANEL)
        rid = rid + r0
        bond[pl.ds(r0, PANEL), :] = jnp.where((cid >= rid) & (rid < own) & (cid < own), r, 0.0)
        return carry

    lax.fori_loop(0, n // PANEL, body, 0)
    rid, cid = places(LANES)
    lower_part = rid > cid
    at = 0
    for i in range(tiles):
        for j in range(i, tiles):
            where = (pl.ds(i * LANES, LANES), pl.ds(j * LANES, LANES))
            tile = bond[where]
            if i == j:
                tile = jnp.where(lower_part, inv0[where], tile)
            packed[pl.ds(at, LANES), :] = tile
            at += LANES


def factor(sizes, site, lower):
    n = lower.shape[-1]
    tiles = n // LANES
    return pl.pallas_call(
        factor_kernel,
        out_shape=[
            jax.ShapeDtypeStruct((n, n), f32),
            jax.ShapeDtypeStruct((tiles * (tiles + 1) // 2 * LANES, LANES), f32),
        ],
        in_specs=[SM, VM, VM],
        out_specs=[VM] * 2,
        scratch_shapes=[
            pltpu.VMEM((n, n), f32),
            pltpu.VMEM((n + PANEL, n), f32),
            pltpu.VMEM((LANES, PANEL), f32),
            pltpu.VMEM((PANEL, n), f32),
            pltpu.VMEM((PANEL, LANES), f32),
            pltpu.VMEM((6 * PANEL, n), bf16),
            pltpu.VMEM((6 * PANEL, n), bf16),
        ],
        compiler_params=params(12),
        name="factor",
    )(sizes, site, lower)


def unpacked(message, n):
    tiles, at, rows = n // LANES, 0, []
    for i in range(tiles):
        row = [jnp.zeros((LANES, LANES), f32)] * i
        for _ in range(i, tiles):
            row.append(message[at : at + LANES, :])
            at += LANES
        rows.append(jnp.concatenate(row, 1))
    both = jnp.concatenate(rows, 0)
    rid, cid = places(n)
    return jnp.where(cid >= rid, both, 0.0), jnp.where(cid < rid, both, 0.0)


def block_inverse(message, n):
    bond, x = unpacked(message, n)
    rid, cid = places(n)
    diagonal = rid == cid
    return jnp.where(diagonal, 1.0 / jnp.where(diagonal & (bond != 0.0), bond, 1.0), x)


def grown_inverse(message, x, size, stop):
    n = x.shape[-1]
    rid, cid = places(n)
    low_tri = unpacked(message, n)[0].T
    while size < stop:
        off = (rid // (2 * size) == cid // (2 * size)) & (rid // size > cid // size)
        part = split3(jnp.where(off, low_tri, 0.0))
        xs = split3(x)
        x = x - dot6(xs, split3(dot6(part, xs)))
        size *= 2
    return x


def upper_rows_kernel(sizes, packed, site, out):
    n = out.shape[-1]
    _, own, _ = own_sizes(sizes)
    x = split3(grown_inverse(packed[...], block_inverse(packed[...], n), PANEL, n))
    rid, cid = places(n)
    out[...] = dot6(split3(jnp.where((cid < own) & (rid < own), site[0, 0], 0.0)), x, 1)


def upper_rows(sizes, packed, site):
    n = site.shape[-1]
    return pl.pallas_call(
        upper_rows_kernel,
        out_shape=jax.ShapeDtypeStruct((n, n), f32),
        in_specs=[SM, VM, VM],
        out_specs=VM,
        compiler_params=params(16),
        name="upper_rows",
    )(sizes, packed, site)


SPLIT_AT = 4 * PANEL


def next_message(near, far):
    odd = lax.rem(lax.axis_index("row"), 2) == 1
    return jnp.where(jnp.broadcast_to(odd, near.shape), far[...], near[...])


def next_inverse_kernel(near, far, out):
    message = next_message(near, far)
    n = out.shape[-1]
    out[...] = grown_inverse(message, block_inverse(message, n), PANEL, SPLIT_AT)


def next_inverse(near, far, n):
    return pl.pallas_call(
        next_inverse_kernel,
        out_shape=jax.ShapeDtypeStruct((n, n), f32),
        in_specs=[VM] * 2,
        out_specs=VM,
        compiler_params=params(16),
        name="next_inverse",
    )(near, far)


def lower_rows_kernel(sizes, near, far, inv, site, top, out, low, sems):
    n = low.shape[-1]
    top_copy = pltpu.make_async_copy(top, out.at[0, 0], sems.at[0])
    top_copy.start()
    q, own, _ = own_sizes(sizes)
    count = lax.axis_size("row")
    after = sizes[jnp.minimum(q + 1, count - 1)]
    after = jnp.where(q + 1 < count, after, 0)
    x = split3(grown_inverse(next_message(near, far), inv[...], SPLIT_AT, n))
    rid, cid = places(n)
    low[...] = dot6(split3(jnp.where((cid < after) & (rid < own), site[0, 1], 0.0)), x, 1)
    low_copy = pltpu.make_async_copy(low, out.at[0, 1], sems.at[1])
    low_copy.start()
    top_copy.wait()
    low_copy.wait()


def lower_rows(sizes, near, far, inv, site, top):
    n = site.shape[-1]
    return pl.pallas_call(
        lower_rows_kernel,
        out_shape=jax.ShapeDtypeStruct((1, 2, n, n), f32),
        in_specs=[SM] + [VM] * 4 + [ANY],
        out_specs=ANY,
        scratch_shapes=[pltpu.VMEM((n, n), f32), pltpu.SemaphoreType.DMA((2,))],
        compiler_params=params(16),
        name="lower_rows",
    )(sizes, near, far, inv, site, top)


def channel(left, a, field, right):
    return dot3(split2(left[0, a]), split2(dot3(field, split2(right))))


def field_of(ref, n):
    return ref[...] if ref.shape[-1] == n else unpacked(ref[...], n)[0]


def moved_terms(field, left, right, base, total):
    f = split2(field)
    for a in range(right.shape[0]):
        total = total + channel(left, base + a, f, right[a])
    return total


def local_kernel(field, near, left, right, right_near, out):
    n = out.shape[-1]
    f = split2(field[...])
    total = jnp.zeros((n, n), f32)
    for a in range(W_DN + W_UP, left.shape[1]):
        total = total + channel(left, a, f, right[0, a])
    odd = lax.rem(lax.axis_index("row"), 2)
    out[...] = moved_terms(field_of(near, n), left, right_near, (1 - odd) * W_DN, total)


def local_terms(field, near, left, right, right_near):
    n = field.shape[-1]
    return pl.pallas_call(
        local_kernel,
        out_shape=jax.ShapeDtypeStruct((n, n), f32),
        in_specs=[VM] * 5,
        out_specs=VM,
        compiler_params=params(16),
        name="local_terms",
    )(field, near, left, right, right_near)


def with_far(sizes, far, left, early, middle, late, part):
    n = part.shape[-1]
    q, own, _ = own_sizes(sizes)
    kind = jnp.broadcast_to(far_kind(q) == 0, (n, n))
    half = early.shape[0]
    total = part[...]
    f = split2(field_of(far, n))
    for a in range(2 * half):
        pair = (early[a], middle[a]) if a < half else (middle[a - half], late[a - half])
        total = total + channel(left, lax.rem(q, 2) * W_DN + a, f, jnp.where(kind, *pair))
    rid, cid = places(n)
    return jnp.where((rid < own) & (cid < own), total, 0.0)


def first_kernel(sizes, far, left, early, middle, late, part, out):
    out[...] = with_far(sizes, far, left, early, middle, late, part)


def first_apply(sizes, far, left, right_far, part):
    n = part.shape[-1]
    return pl.pallas_call(
        first_kernel,
        out_shape=jax.ShapeDtypeStruct((n, n), f32),
        in_specs=[SM] + [VM] * 6,
        out_specs=VM,
        compiler_params=params(16),
        name="first",
    )(sizes, far, left, *right_far, part)


def second_kernel(sizes, far, left, early, middle, late, part, bond, applied, out, spread):
    twice = with_far(sizes, far, left, early, middle, late, part)
    out[...] = twice
    basis = (bond[...], time_step * applied[...], (0.5 * time_step * time_step) * twice)
    sums = []
    for i in range(3):
        for j in range(i, 3):
            line = jnp.sum(basis[i] * basis[j], 0, keepdims=True)
            sums.append(sum(line[:, t : t + LANES] for t in range(0, line.shape[1], LANES)))
    block = jnp.concatenate(sums + [jnp.zeros((2, LANES), f32)], 0)
    for i in range(spread.shape[0]):
        spread[i] = block


def second_apply(sizes, far, left, right_far, part, bond, applied, count):
    n = part.shape[-1]
    return pl.pallas_call(
        second_kernel,
        out_shape=[
            jax.ShapeDtypeStruct((n, n), f32),
            jax.ShapeDtypeStruct((count, 8, LANES), f32),
        ],
        in_specs=[SM] + [VM] * 8,
        out_specs=[VM, VM],
        compiler_params=params(16),
        name="second",
    )(sizes, far, left, *right_far, part, bond, applied)


def final_kernel(gathered, bond, applied, twice, out):
    sums = jnp.sum(jnp.sum(gathered[...], 0), 1, keepdims=True)
    bb, ba, bt, aa, at, tt = (jnp.broadcast_to(sums[i : i + 1, :], (1, bond.shape[-1])) for i in range(6))
    rate = ba / bb
    c0 = 1.0 - rate + 0.5 * rate * rate
    c1 = 1.0 - rate
    norm = c0 * (c0 * bb + 2.0 * (c1 * ba + bt)) + c1 * (c1 * aa + 2.0 * at) + tt
    scale = jnp.sqrt(bb / norm)
    steps = (c0 * scale, (c1 * time_step) * scale, (0.5 * time_step * time_step) * scale)
    out[0] = steps[0] * bond[...] + steps[1] * applied[...] + steps[2] * twice[...]


def final(gathered, bond, applied, twice):
    n = bond.shape[-1]
    return pl.pallas_call(
        final_kernel,
        out_shape=jax.ShapeDtypeStruct((1, n, n), f32),
        in_specs=[VM] * 4,
        out_specs=VM,
        compiler_params=params(4),
        name="final",
    )(gathered, bond, applied, twice)


def shifted_by(value, steps):
    count = lax.axis_size("row")
    first, last = max(0, -steps), min(count, count - steps)
    return lax.ppermute(value, "row", [(source, source + steps) for source in range(first, last)])


def swapped(value, first, step=2):
    count = lax.axis_size("row")
    pairs = [(i, i + 1) for i in range(first, count - 1, step)]
    return lax.ppermute(value, "row", pairs + [(j, i) for i, j in pairs])


def bond_update(site, left, right, sizes):
    count = lax.axis_size("row")
    source, early, middle, late = take_far(site, right)
    early = swapped(early, 3, 4)
    lower = shifted_by(source, 1)
    middle = swapped(middle, 1)
    late = swapped(late, 1, 4)
    right_far = (early, middle, late)
    to_near = take_near(right)
    right_near = swapped(to_near, 0)
    bond, packed = factor(sizes, site, lower)
    bond_far = swapped(packed, 1)
    bond_near = swapped(packed, 0)
    top = upper_rows(sizes, packed, site)
    part = local_terms(bond, bond_near, left, right, right_near)
    applied = first_apply(sizes, bond_far, left, right_far, part)
    far = swapped(applied, 1)
    near = swapped(applied, 0)
    inv = next_inverse(bond_near, bond_far, bond.shape[-1])
    part = local_terms(applied, near, left, right, right_near)
    twice, spread = second_apply(sizes, far, left, right_far, part, bond, applied, count)
    gathered = lax.all_to_all(spread, "row", 0, 0, tiled=True)
    left_out = lower_rows(sizes, bond_near, bond_far, inv, site, top)
    bond_out = final(gathered, bond, applied, twice)
    return left_out, bond_out


def solution(mesh):
    placed = (
        P(("real", "row"), None, None, None),
        P(("real", "row"), None, None, None),
        P(("real", "row"), None, None, None),
        P("real"),
    )
    return jax.shard_map(
        bond_update,
        mesh=mesh,
        in_specs=placed,
        out_specs=(P(("real", "row"), None, None, None), P(("real", "row"), None, None)),
        check_vma=False,
    )
```

```python
import jax
import jax.numpy as jnp
from jax import lax
from jax.experimental import pallas as pl
from jax.experimental.pallas import tpu as pltpu
from jax.sharding import PartitionSpec as P

W_DN = 4
W_UP = 4
PANEL = 16
LANES = 128

f32, bf16 = jnp.float32, jnp.bfloat16
time_step = 0.15

VM = pl.BlockSpec(memory_space=pltpu.VMEM)
SM = pl.BlockSpec(memory_space=pltpu.SMEM)
ANY = pl.BlockSpec(memory_space=pl.ANY)
HB = pl.BlockSpec(memory_space=pltpu.HBM)


def params(mib):
    return pltpu.CompilerParams(vmem_limit_bytes=mib << 20)


def split2(x):
    hi = x.astype(bf16)
    return hi, (x - hi.astype(f32)).astype(bf16)


def split3(x):
    hi = x.astype(bf16)
    rest = x - hi.astype(f32)
    mid = rest.astype(bf16)
    return hi, mid, (rest - mid.astype(f32)).astype(bf16)


def dot(a, b, ca=1, cb=0):
    return lax.dot_general(a, b, (((ca,), (cb,)), ((), ())), preferred_element_type=f32)


def dot3(a, b):
    ah, al = a
    bh, bl = b
    return dot(ah, bh) + dot(al, bh) + dot(ah, bl)


def dot6(a, b, cb=0):
    ah, am, al = a
    bh, bm, bl = b
    pairs = ((ah, bh), (ah, bm), (am, bh), (am, bm), (ah, bl), (al, bh))
    return sum(dot(x, y, 1, cb) for x, y in pairs)


def places(n, rows=None):
    shape = (n if rows is None else rows, n)
    return lax.broadcasted_iota(jnp.int32, shape, 0), lax.broadcasted_iota(jnp.int32, shape, 1)


def own_sizes(sizes):
    q = lax.axis_index("row")
    return q, sizes[q], sizes[jnp.maximum(q - 1, 0)]


def far_kind(q):
    return lax.rem((q + 1) // 2, 2)


def first_far(q):
    return (1 - lax.rem(q, 2)) * W_DN


def run_copies(copies):
    for copy in copies:
        copy.start()
    for copy in copies:
        copy.wait()


def take_early_kernel(site, right, source, early, sems):
    half = early.shape[0]
    start = first_far(lax.axis_index("row"))
    run_copies(
        (
            pltpu.make_async_copy(site.at[0, 1], source, sems.at[0]),
            pltpu.make_async_copy(right.at[0, pl.ds(start, half)], early, sems.at[1]),
        )
    )


def take_rest_kernel(right, middle, late, near, sems):
    q = lax.axis_index("row")
    half = late.shape[0]
    start = first_far(q)
    turn = jnp.where(far_kind(q) == 0, start + half, start)
    run_copies(
        (
            pltpu.make_async_copy(right.at[0, pl.ds(turn, half)], middle, sems.at[0]),
            pltpu.make_async_copy(right.at[0, pl.ds(start + half, half)], late, sems.at[1]),
            pltpu.make_async_copy(right.at[0, pl.ds(lax.rem(q, 2) * W_DN, W_DN)], near, sems.at[2]),
        )
    )


def in_hbm(x):
    return pltpu.with_memory_space_constraint(x, pltpu.HBM)


def take_early(site, right):
    n = right.shape[-1]
    return pl.pallas_call(
        take_early_kernel,
        out_shape=[jax.ShapeDtypeStruct((n, n), f32), jax.ShapeDtypeStruct((W_UP // 2, n, n), f32)],
        in_specs=[HB] * 2,
        out_specs=[ANY] * 2,
        scratch_shapes=[pltpu.SemaphoreType.DMA((2,))],
        compiler_params=params(4),
        name="take_early",
    )(in_hbm(site), in_hbm(right))


def take_rest(right):
    n = right.shape[-1]
    return pl.pallas_call(
        take_rest_kernel,
        out_shape=[jax.ShapeDtypeStruct((W_UP // 2, n, n), f32)] * 2 + [jax.ShapeDtypeStruct((W_DN, n, n), f32)],
        in_specs=[HB],
        out_specs=[ANY] * 3,
        scratch_shapes=[pltpu.SemaphoreType.DMA((3,))],
        compiler_params=params(4),
        name="take_rest",
    )(in_hbm(right))


def factor_kernel(sizes, site, lower, bond, packed, mask, inv0, work, turn, rows, erows, lstack, rstack):
    n = lower.shape[-1]
    _, own, prev = own_sizes(sizes)
    row_id, col_id = places(n)
    live_col = col_id < own
    top = jnp.where(live_col & (row_id < own), site[0, 0], 0.0)
    bot = jnp.where(live_col & (row_id < prev), lower[...], 0.0)
    mask[...] = jnp.where(live_col & (row_id < own), 1.0, 0.0)
    gram = jnp.where((row_id == col_id) & (row_id >= own), 1.0, 0.0)
    for part in (top, bot):
        gram = gram + dot6(split3(part.T), split3(part))
    work[pl.ds(0, n), :] = gram
    work[pl.ds(n, PANEL), :] = jnp.zeros((PANEL, n), f32)
    lstack[...] = jnp.zeros(lstack.shape, bf16)
    rstack[...] = jnp.zeros(rstack.shape, bf16)
    inv0[...] = jnp.zeros((n, n), f32)
    lane = lax.broadcasted_iota(jnp.int32, (PANEL, LANES), 1)
    sub = lax.broadcasted_iota(jnp.int32, (PANEL, LANES), 0)
    tiles = n // LANES

    def body(p, carry):
        r0 = pl.multiple_of(p * PANEL, PANEL)
        tile = pl.multiple_of((r0 // LANES) * LANES, LANES)
        off = r0 - tile
        after = r0 + PANEL
        ntile = pl.multiple_of(jnp.minimum((after // LANES) * LANES, n - LANES), LANES)
        noff = pl.multiple_of(lax.rem(after, LANES), PANEL)
        w = work[pl.ds(r0, PANEL), :]
        diag = work[pl.ds(r0, PANEL), pl.ds(tile, LANES)]
        turn[...] = work[pl.ds(r0, PANEL), pl.ds(ntile, LANES)].T
        update = dot(lstack[...], rstack[...], 0, 0)
        ahead = turn[pl.ds(noff, PANEL), :]
        here, there = [], []
        for j in range(PANEL):
            at = jnp.full((PANEL, LANES), off + j, jnp.int32)
            here.append(jnp.take_along_axis(diag, at, axis=1, mode="promise_in_bounds"))
            there.append(jnp.broadcast_to(ahead[:, j : j + 1], (PANEL, LANES)))
        ext = jnp.where(lane == off + sub, 1.0, 0.0)
        acc = jnp.zeros((PANEL, n), f32)
        for k in range(PANEL):
            scale = lax.rsqrt(jnp.broadcast_to(here[k][k : k + 1, :], (PANEL, LANES)))
            a = here[k] * scale
            b = there[k] * scale
            rk = w[k : k + 1, :] * jnp.concatenate([scale[:1]] * tiles, 1)
            ek = ext[k : k + 1, :] * scale[:1]
            rows[k : k + 1, :] = rk
            erows[k : k + 1, :] = ek
            spread = jnp.broadcast_to(rk, (PANEL, n))
            acc = acc + jnp.concatenate([b] * tiles, 1) * spread
            if k + 1 < PANEL:
                w = w - jnp.concatenate([a] * tiles, 1) * spread
                ext = ext - a * jnp.broadcast_to(ek, (PANEL, LANES))
            for j in range(k + 1, PANEL):
                s = jnp.broadcast_to(a[j : j + 1, :], (PANEL, LANES))
                here[j] = here[j] - a * s
                there[j] = there[j] - b * s
        work[pl.ds(0, n), :] = work[pl.ds(0, n), :] - update
        work[pl.ds(after, PANEL), :] = work[pl.ds(after, PANEL), :] - acc
        r = rows[...]
        inv0[pl.ds(r0, PANEL), pl.ds(tile, LANES)] = erows[...]
        h, m, l = split3(r)
        for i, (x, y) in enumerate(((h, h), (m, h), (h, m), (m, m), (l, h), (h, l))):
            lstack[pl.ds(i * PANEL, PANEL), :] = x
            rstack[pl.ds(i * PANEL, PANEL), :] = y
        rid, cid = places(n, PANEL)
        rid = rid + r0
        bond[pl.ds(r0, PANEL), :] = jnp.where((cid >= rid) & (rid < own) & (cid < own), r, 0.0)
        return carry

    lax.fori_loop(0, n // PANEL, body, 0)
    rid, cid = places(LANES)
    diagonal = []
    for i in range(tiles):
        where = (pl.ds(i * LANES, LANES), pl.ds(i * LANES, LANES))
        diagonal.append(jnp.where(rid > cid, inv0[where], bond[where]))
    at = 0
    for part in fold(diagonal):
        packed[pl.ds(at, part.shape[0]), :] = part
        at += part.shape[0]
    for i in range(tiles):
        for j in range(i + 1, tiles):
            packed[pl.ds(at, LANES), :] = bond[pl.ds(i * LANES, LANES), pl.ds(j * LANES, LANES)]
            at += LANES


def fold(diagonal):
    half = LANES // 2
    low = lax.broadcasted_iota(jnp.int32, (half, LANES), 1) < half
    parts = []
    for i in range(0, len(diagonal) - 1, 2):
        first, second = diagonal[i], diagonal[i + 1]
        parts.append(first[:half])
        parts.append(jnp.where(low, pltpu.roll(second[:half], half, 1), first[half:]))
        parts.append(jnp.where(low, second[:half], second[half:]))
    return parts + diagonal[len(diagonal) - len(diagonal) % 2 :]


def unfold(message, tiles):
    half = LANES // 2
    low = lax.broadcasted_iota(jnp.int32, (half, LANES), 1) < half
    diagonal, at = [], 0
    for _ in range(0, tiles - 1, 2):
        a, b, c = (message[at + i * half : at + (i + 1) * half, :] for i in range(3))
        diagonal.append(jnp.concatenate([a, jnp.where(low, 0.0, b)], 0))
        diagonal.append(jnp.concatenate([jnp.where(low, c, pltpu.roll(b, half, 1)), jnp.where(low, 0.0, c)], 0))
        at += 3 * half
    if tiles % 2:
        diagonal.append(message[at : at + LANES, :])
        at += LANES
    return diagonal, at


def factor(sizes, site, lower):
    n = lower.shape[-1]
    tiles = n // LANES
    return pl.pallas_call(
        factor_kernel,
        out_shape=[
            jax.ShapeDtypeStruct((n, n), f32),
            jax.ShapeDtypeStruct((tiles * (tiles + 1) // 2 * LANES - tiles // 2 * (LANES // 2), LANES), f32),
            jax.ShapeDtypeStruct((n, n), f32),
        ],
        in_specs=[SM, VM, VM],
        out_specs=[VM] * 3,
        scratch_shapes=[
            pltpu.VMEM((n, n), f32),
            pltpu.VMEM((n + PANEL, n), f32),
            pltpu.VMEM((LANES, PANEL), f32),
            pltpu.VMEM((PANEL, n), f32),
            pltpu.VMEM((PANEL, LANES), f32),
            pltpu.VMEM((6 * PANEL, n), bf16),
            pltpu.VMEM((6 * PANEL, n), bf16),
        ],
        compiler_params=params(12),
        name="factor",
    )(sizes, site, lower)


def unpacked(message, n):
    tiles = n // LANES
    diagonal, at = unfold(message, tiles)
    rows = []
    for i in range(tiles):
        row = [jnp.zeros((LANES, LANES), f32)] * i + [diagonal[i]]
        for _ in range(i + 1, tiles):
            row.append(message[at : at + LANES, :])
            at += LANES
        rows.append(jnp.concatenate(row, 1))
    both = jnp.concatenate(rows, 0)
    rid, cid = places(n)
    return jnp.where(cid >= rid, both, 0.0), jnp.where(cid < rid, both, 0.0)


def block_inverse(message, n):
    bond, x = unpacked(message, n)
    rid, cid = places(n)
    diagonal = rid == cid
    return jnp.where(diagonal, 1.0 / jnp.where(diagonal & (bond != 0.0), bond, 1.0), x)


def grown_inverse(message, x, size, stop):
    n = x.shape[-1]
    rid, cid = places(n)
    low_tri = unpacked(message, n)[0].T
    while size < stop:
        off = (rid // (2 * size) == cid // (2 * size)) & (rid // size > cid // size)
        part = split3(jnp.where(off, low_tri, 0.0))
        xs = split3(x)
        x = x - dot6(xs, split3(dot6(part, xs)))
        size *= 2
    return x


def upper_rows_kernel(sizes, packed, site, out):
    n = out.shape[-1]
    _, own, _ = own_sizes(sizes)
    x = split3(grown_inverse(packed[...], block_inverse(packed[...], n), PANEL, n))
    rid, cid = places(n)
    out[...] = dot6(split3(jnp.where((cid < own) & (rid < own), site[0, 0], 0.0)), x, 1)


def upper_rows(sizes, packed, site):
    n = site.shape[-1]
    return pl.pallas_call(
        upper_rows_kernel,
        out_shape=jax.ShapeDtypeStruct((n, n), f32),
        in_specs=[SM, VM, VM],
        out_specs=VM,
        compiler_params=params(16),
        name="upper_rows",
    )(sizes, packed, site)


SPLIT_AT = 4 * PANEL


def next_message(near, far):
    odd = lax.rem(lax.axis_index("row"), 2) == 1
    return jnp.where(jnp.broadcast_to(odd, near.shape), far[...], near[...])


def next_inverse_kernel(near, far, bond, applied, out, known):
    b, a = bond[...], time_step * applied[...]
    known[...] = lane_sums(((b, b), (b, a), (a, a)), 0)
    message = next_message(near, far)
    n = out.shape[-1]
    out[...] = grown_inverse(message, block_inverse(message, n), PANEL, SPLIT_AT)


def next_inverse(near, far, bond, applied):
    n = bond.shape[-1]
    return pl.pallas_call(
        next_inverse_kernel,
        out_shape=[jax.ShapeDtypeStruct((n, n), f32), jax.ShapeDtypeStruct((1, LANES), f32)],
        in_specs=[VM] * 4,
        out_specs=[VM] * 2,
        compiler_params=params(16),
        name="next_inverse",
    )(near, far, bond, applied)


def lower_rows_kernel(sizes, near, far, inv, site, top, out, low, sems):
    n = low.shape[-1]
    top_copy = pltpu.make_async_copy(top, out.at[0, 0], sems.at[0])
    top_copy.start()
    q, own, _ = own_sizes(sizes)
    count = lax.axis_size("row")
    after = sizes[jnp.minimum(q + 1, count - 1)]
    after = jnp.where(q + 1 < count, after, 0)
    x = split3(grown_inverse(next_message(near, far), inv[...], SPLIT_AT, n))
    rid, cid = places(n)
    low[...] = dot6(split3(jnp.where((cid < after) & (rid < own), site[0, 1], 0.0)), x, 1)
    low_copy = pltpu.make_async_copy(low, out.at[0, 1], sems.at[1])
    low_copy.start()
    top_copy.wait()
    low_copy.wait()


def lower_rows(sizes, near, far, inv, site, top):
    n = site.shape[-1]
    return pl.pallas_call(
        lower_rows_kernel,
        out_shape=jax.ShapeDtypeStruct((1, 2, n, n), f32),
        in_specs=[SM] + [VM] * 4 + [ANY],
        out_specs=ANY,
        scratch_shapes=[pltpu.VMEM((n, n), f32), pltpu.SemaphoreType.DMA((2,))],
        compiler_params=params(16),
        name="lower_rows",
    )(sizes, near, far, inv, site, top)


def channel(left, a, field, right):
    return dot3(split2(left[0, a]), split2(dot3(field, split2(right))))


def field_of(ref, n):
    return ref[...] if ref.shape[-1] == n else unpacked(ref[...], n)[0]


def moved_terms(field, left, right, base, total):
    f = split2(field)
    for a in range(right.shape[0]):
        total = total + channel(left, base + a, f, right[a])
    return total


def local_kernel(field, near, left, right, right_near, out):
    n = out.shape[-1]
    f = split2(field[...])
    total = jnp.zeros((n, n), f32)
    for a in range(W_DN + W_UP, left.shape[1]):
        total = total + channel(left, a, f, right[0, a])
    odd = lax.rem(lax.axis_index("row"), 2)
    out[...] = moved_terms(field_of(near, n), left, right_near, (1 - odd) * W_DN, total)


def local_terms(field, near, left, right, right_near):
    n = field.shape[-1]
    return pl.pallas_call(
        local_kernel,
        out_shape=jax.ShapeDtypeStruct((n, n), f32),
        in_specs=[VM] * 5,
        out_specs=VM,
        compiler_params=params(16),
        name="local_terms",
    )(field, near, left, right, right_near)


def with_far(mask, far, left, early, middle, late, part):
    n = part.shape[-1]
    q = lax.axis_index("row")
    kind = jnp.broadcast_to(far_kind(q) == 0, (n, n))
    half = early.shape[0]
    total = part[...]
    f = split2(field_of(far, n))
    for a in range(2 * half):
        pair = (early[a], middle[a]) if a < half else (middle[a - half], late[a - half])
        total = total + channel(left, lax.rem(q, 2) * W_DN + a, f, jnp.where(kind, *pair))
    return jnp.where(mask[...] > 0.0, total, 0.0)


def first_kernel(mask, far, left, early, middle, late, part, out):
    out[...] = with_far(mask, far, left, early, middle, late, part)


def first_apply(mask, far, left, right_far, part):
    n = part.shape[-1]
    return pl.pallas_call(
        first_kernel,
        out_shape=jax.ShapeDtypeStruct((n, n), f32),
        in_specs=[VM] * 7,
        out_specs=VM,
        compiler_params=params(16),
        name="first",
    )(mask, far, left, *right_far, part)


def lane_sums(pairs, first):
    lane = lax.broadcasted_iota(jnp.int32, (1, LANES), 1)
    row = jnp.zeros((1, LANES), f32)
    for i, (x, y) in enumerate(pairs):
        line = jnp.sum(jnp.sum(x * y, 0, keepdims=True), 1, keepdims=True)
        row = row + jnp.where(lane == first + i, line, 0.0)
    return row


def second_kernel(mask, far, left, early, middle, late, part, bond, applied, known, out, spread):
    twice = with_far(mask, far, left, early, middle, late, part)
    out[...] = twice
    b, a = bond[...], time_step * applied[...]
    t = (0.5 * time_step * time_step) * twice
    row = known[...] + lane_sums(((b, t), (a, t), (t, t)), 3)
    for i in range(spread.shape[0]):
        spread[i] = row


def second_apply(mask, far, left, right_far, part, bond, applied, known, count):
    n = part.shape[-1]
    return pl.pallas_call(
        second_kernel,
        out_shape=[
            jax.ShapeDtypeStruct((n, n), f32),
            pltpu.VMEM((count, 1, LANES), f32),
        ],
        in_specs=[VM] * 10,
        out_specs=[VM, VM],
        compiler_params=params(16),
        name="second",
    )(mask, far, left, *right_far, part, bond, applied, known)


def final_kernel(gathered, bond, applied, twice, out):
    sums = jnp.sum(gathered[...], 0)
    bb, ba, aa, bt, at, tt = (jnp.broadcast_to(sums[:, i : i + 1], (1, bond.shape[-1])) for i in range(6))
    rate = ba / bb
    c0 = 1.0 - rate + 0.5 * rate * rate
    c1 = 1.0 - rate
    norm = c0 * (c0 * bb + 2.0 * (c1 * ba + bt)) + c1 * (c1 * aa + 2.0 * at) + tt
    scale = jnp.sqrt(bb / norm)
    steps = (c0 * scale, (c1 * time_step) * scale, (0.5 * time_step * time_step) * scale)
    out[0] = steps[0] * bond[...] + steps[1] * applied[...] + steps[2] * twice[...]


def final(gathered, bond, applied, twice):
    n = bond.shape[-1]
    return pl.pallas_call(
        final_kernel,
        out_shape=jax.ShapeDtypeStruct((1, n, n), f32),
        in_specs=[VM] * 4,
        out_specs=VM,
        compiler_params=params(4),
        name="final",
    )(gathered, bond, applied, twice)


def shifted_by(value, steps):
    count = lax.axis_size("row")
    first, last = max(0, -steps), min(count, count - steps)
    return lax.ppermute(value, "row", [(source, source + steps) for source in range(first, last)])


def swapped(value, first, step=2):
    count = lax.axis_size("row")
    pairs = [(i, i + 1) for i in range(first, count - 1, step)]
    return lax.ppermute(value, "row", pairs + [(j, i) for i, j in pairs])


def bond_update(site, left, right, sizes):
    count = lax.axis_size("row")
    source, early = take_early(site, right)
    early = swapped(early, 3, 4)
    lower = shifted_by(source, 1)
    middle, late, to_near = take_rest(right)
    middle = swapped(middle, 1)
    late = swapped(late, 1, 4)
    right_far = (early, middle, late)
    right_near = swapped(to_near, 0)
    bond, packed, mask = factor(sizes, site, lower)
    bond_far = swapped(packed, 1)
    bond_near = swapped(packed, 0)
    top = upper_rows(sizes, packed, site)
    part = local_terms(bond, bond_near, left, right, right_near)
    applied = first_apply(mask, bond_far, left, right_far, part)
    far = swapped(applied, 1)
    near = swapped(applied, 0)
    inv, known = next_inverse(bond_near, bond_far, bond, applied)
    part = local_terms(applied, near, left, right, right_near)
    twice, spread = second_apply(mask, far, left, right_far, part, bond, applied, known, count)
    gathered = lax.all_to_all(spread, "row", 0, 0, tiled=True)
    left_out = lower_rows(sizes, bond_near, bond_far, inv, site, top)
    bond_out = final(gathered, bond, applied, twice)
    return left_out, bond_out


def solution(mesh):
    placed = (
        P(("real", "row"), None, None, None),
        P(("real", "row"), None, None, None),
        P(("real", "row"), None, None, None),
        P("real"),
    )
    return jax.shard_map(
        bond_update,
        mesh=mesh,
        in_specs=placed,
        out_specs=(P(("real", "row"), None, None, None), P(("real", "row"), None, None)),
        check_vma=False,
    )
```

```python
import jax
import jax.numpy as jnp
from jax import lax
from jax.experimental import pallas as pl
from jax.experimental.pallas import tpu as pltpu
from jax.sharding import PartitionSpec as P

W_DN = 4
W_UP = 4
PANEL = 16
CHUNKS = 2
LANES = 128

f32, bf16 = jnp.float32, jnp.bfloat16
time_step = 0.15

VM = pl.BlockSpec(memory_space=pltpu.VMEM)
SM = pl.BlockSpec(memory_space=pltpu.SMEM)
ANY = pl.BlockSpec(memory_space=pl.ANY)
HB = pl.BlockSpec(memory_space=pltpu.HBM)


def params(mib):
    return pltpu.CompilerParams(vmem_limit_bytes=mib << 20)


def split2(x):
    hi = x.astype(bf16)
    return hi, (x - hi.astype(f32)).astype(bf16)


def split3(x):
    hi = x.astype(bf16)
    rest = x - hi.astype(f32)
    mid = rest.astype(bf16)
    return hi, mid, (rest - mid.astype(f32)).astype(bf16)


def dot(a, b, ca=1, cb=0):
    return lax.dot_general(a, b, (((ca,), (cb,)), ((), ())), preferred_element_type=f32)


def dot3(a, b):
    ah, al = a
    bh, bl = b
    return dot(ah, bh) + dot(al, bh) + dot(ah, bl)


def dot6(a, b, cb=0):
    ah, am, al = a
    bh, bm, bl = b
    pairs = ((ah, bh), (ah, bm), (am, bh), (am, bm), (ah, bl), (al, bh))
    return sum(dot(x, y, 1, cb) for x, y in pairs)


def places(n, rows=None):
    shape = (n if rows is None else rows, n)
    return lax.broadcasted_iota(jnp.int32, shape, 0), lax.broadcasted_iota(jnp.int32, shape, 1)


def own_sizes(sizes):
    q = lax.axis_index("row")
    return q, sizes[q], sizes[jnp.maximum(q - 1, 0)]


def far_kind(q):
    return lax.rem((q + 1) // 2, 2)


def first_far(q):
    return (1 - lax.rem(q, 2)) * W_DN


def run_copies(copies):
    for copy in copies:
        copy.start()
    for copy in copies:
        copy.wait()


def take_early_kernel(site, right, source, early, sems):
    half = early.shape[0]
    start = first_far(lax.axis_index("row"))
    run_copies(
        (
            pltpu.make_async_copy(site.at[0, 1], source, sems.at[0]),
            pltpu.make_async_copy(right.at[0, pl.ds(start, half)], early, sems.at[1]),
        )
    )


def take_rest_kernel(right, middle, late, near, sems):
    q = lax.axis_index("row")
    half = late.shape[0]
    start = first_far(q)
    turn = jnp.where(far_kind(q) == 0, start + half, start)
    run_copies(
        (
            pltpu.make_async_copy(right.at[0, pl.ds(turn, half)], middle, sems.at[0]),
            pltpu.make_async_copy(right.at[0, pl.ds(start + half, half)], late, sems.at[1]),
            pltpu.make_async_copy(right.at[0, pl.ds(lax.rem(q, 2) * W_DN, W_DN)], near, sems.at[2]),
        )
    )


def in_hbm(x):
    return pltpu.with_memory_space_constraint(x, pltpu.HBM)


def take_early(site, right):
    n = right.shape[-1]
    return pl.pallas_call(
        take_early_kernel,
        out_shape=[jax.ShapeDtypeStruct((n, n), f32), jax.ShapeDtypeStruct((W_UP // 2, n, n), f32)],
        in_specs=[HB] * 2,
        out_specs=[ANY] * 2,
        scratch_shapes=[pltpu.SemaphoreType.DMA((2,))],
        compiler_params=params(4),
        name="take_early",
    )(in_hbm(site), in_hbm(right))


def take_rest(right):
    n = right.shape[-1]
    return pl.pallas_call(
        take_rest_kernel,
        out_shape=[jax.ShapeDtypeStruct((W_UP // 2, n, n), f32)] * 2 + [jax.ShapeDtypeStruct((W_DN, n, n), f32)],
        in_specs=[HB],
        out_specs=[ANY] * 3,
        scratch_shapes=[pltpu.SemaphoreType.DMA((3,))],
        compiler_params=params(4),
        name="take_rest",
    )(in_hbm(right))


def factor_kernel(sizes, site, lower, bond, packed, mask, inv0, work, turn, rows, erows, lstack, rstack):
    n = lower.shape[-1]
    _, own, prev = own_sizes(sizes)
    row_id, col_id = places(n)
    live_col = col_id < own
    top = jnp.where(live_col & (row_id < own), site[0, 0], 0.0)
    bot = jnp.where(live_col & (row_id < prev), lower[...], 0.0)
    mask[...] = jnp.where(live_col & (row_id < own), 1.0, 0.0)
    gram = jnp.where((row_id == col_id) & (row_id >= own), 1.0, 0.0)
    for part in (top, bot):
        gram = gram + dot6(split3(part.T), split3(part))
    work[pl.ds(0, n), :] = gram
    work[pl.ds(n, PANEL), :] = jnp.zeros((PANEL, n), f32)
    lstack[...] = jnp.zeros(lstack.shape, bf16)
    rstack[...] = jnp.zeros(rstack.shape, bf16)
    inv0[...] = jnp.zeros((n, n), f32)
    lane = lax.broadcasted_iota(jnp.int32, (PANEL, LANES), 1)
    sub = lax.broadcasted_iota(jnp.int32, (PANEL, LANES), 0)
    tiles = n // LANES

    def body(p, carry):
        r0 = pl.multiple_of(p * PANEL, PANEL)
        tile = pl.multiple_of((r0 // LANES) * LANES, LANES)
        off = r0 - tile
        after = r0 + PANEL
        ntile = pl.multiple_of(jnp.minimum((after // LANES) * LANES, n - LANES), LANES)
        noff = pl.multiple_of(lax.rem(after, LANES), PANEL)
        w = work[pl.ds(r0, PANEL), :]
        diag = work[pl.ds(r0, PANEL), pl.ds(tile, LANES)]
        turn[...] = work[pl.ds(r0, PANEL), pl.ds(ntile, LANES)].T
        update = dot(lstack[...], rstack[...], 0, 0)
        ahead = turn[pl.ds(noff, PANEL), :]
        here, there = [], []
        for j in range(PANEL):
            at = jnp.full((PANEL, LANES), off + j, jnp.int32)
            here.append(jnp.take_along_axis(diag, at, axis=1, mode="promise_in_bounds"))
            there.append(jnp.broadcast_to(ahead[:, j : j + 1], (PANEL, LANES)))
        ext = jnp.where(lane == off + sub, 1.0, 0.0)
        acc = jnp.zeros((PANEL, n), f32)
        for k in range(PANEL):
            scale = lax.rsqrt(jnp.broadcast_to(here[k][k : k + 1, :], (PANEL, LANES)))
            a = here[k] * scale
            b = there[k] * scale
            rk = w[k : k + 1, :] * jnp.concatenate([scale[:1]] * tiles, 1)
            ek = ext[k : k + 1, :] * scale[:1]
            rows[k : k + 1, :] = rk
            erows[k : k + 1, :] = ek
            spread = jnp.broadcast_to(rk, (PANEL, n))
            acc = acc + jnp.concatenate([b] * tiles, 1) * spread
            if k + 1 < PANEL:
                w = w - jnp.concatenate([a] * tiles, 1) * spread
                ext = ext - a * jnp.broadcast_to(ek, (PANEL, LANES))
            for j in range(k + 1, PANEL):
                s = jnp.broadcast_to(a[j : j + 1, :], (PANEL, LANES))
                here[j] = here[j] - a * s
                there[j] = there[j] - b * s
        work[pl.ds(0, n), :] = work[pl.ds(0, n), :] - update
        work[pl.ds(after, PANEL), :] = work[pl.ds(after, PANEL), :] - acc
        r = rows[...]
        inv0[pl.ds(r0, PANEL), pl.ds(tile, LANES)] = erows[...]
        h, m, l = split3(r)
        for i, (x, y) in enumerate(((h, h), (m, h), (h, m), (m, m), (l, h), (h, l))):
            lstack[pl.ds(i * PANEL, PANEL), :] = x
            rstack[pl.ds(i * PANEL, PANEL), :] = y
        rid, cid = places(n, PANEL)
        rid = rid + r0
        bond[pl.ds(r0, PANEL), :] = jnp.where((cid >= rid) & (rid < own) & (cid < own), r, 0.0)
        return carry

    lax.fori_loop(0, n // PANEL, body, 0)
    rid, cid = places(LANES)
    diagonal = []
    for i in range(tiles):
        where = (pl.ds(i * LANES, LANES), pl.ds(i * LANES, LANES))
        diagonal.append(jnp.where(rid > cid, inv0[where], bond[where]))
    at = 0
    for part in fold(diagonal):
        packed[pl.ds(at, part.shape[0]), :] = part
        at += part.shape[0]
    for i in range(tiles):
        for j in range(i + 1, tiles):
            packed[pl.ds(at, LANES), :] = bond[pl.ds(i * LANES, LANES), pl.ds(j * LANES, LANES)]
            at += LANES


def fold(diagonal):
    half = LANES // 2
    low = lax.broadcasted_iota(jnp.int32, (half, LANES), 1) < half
    parts = []
    for i in range(0, len(diagonal) - 1, 2):
        first, second = diagonal[i], diagonal[i + 1]
        parts.append(first[:half])
        parts.append(jnp.where(low, pltpu.roll(second[:half], half, 1), first[half:]))
        parts.append(jnp.where(low, second[:half], second[half:]))
    return parts + diagonal[len(diagonal) - len(diagonal) % 2 :]


def unfold(message, tiles):
    half = LANES // 2
    low = lax.broadcasted_iota(jnp.int32, (half, LANES), 1) < half
    diagonal, at = [], 0
    for _ in range(0, tiles - 1, 2):
        a, b, c = (message[at + i * half : at + (i + 1) * half, :] for i in range(3))
        diagonal.append(jnp.concatenate([a, jnp.where(low, 0.0, b)], 0))
        diagonal.append(jnp.concatenate([jnp.where(low, c, pltpu.roll(b, half, 1)), jnp.where(low, 0.0, c)], 0))
        at += 3 * half
    if tiles % 2:
        diagonal.append(message[at : at + LANES, :])
        at += LANES
    return diagonal, at


def factor(sizes, site, lower):
    n = lower.shape[-1]
    tiles = n // LANES
    return pl.pallas_call(
        factor_kernel,
        out_shape=[
            jax.ShapeDtypeStruct((n, n), f32),
            jax.ShapeDtypeStruct((tiles * (tiles + 1) // 2 * LANES - tiles // 2 * (LANES // 2), LANES), f32),
            jax.ShapeDtypeStruct((n, n), f32),
        ],
        in_specs=[SM, VM, VM],
        out_specs=[VM] * 3,
        scratch_shapes=[
            pltpu.VMEM((n, n), f32),
            pltpu.VMEM((n + PANEL, n), f32),
            pltpu.VMEM((LANES, PANEL), f32),
            pltpu.VMEM((PANEL, n), f32),
            pltpu.VMEM((PANEL, LANES), f32),
            pltpu.VMEM((6 * PANEL, n), bf16),
            pltpu.VMEM((6 * PANEL, n), bf16),
        ],
        compiler_params=params(12),
        name="factor",
    )(sizes, site, lower)


def unpacked(message, n):
    tiles = n // LANES
    diagonal, at = unfold(message, tiles)
    rows = []
    for i in range(tiles):
        row = [jnp.zeros((LANES, LANES), f32)] * i + [diagonal[i]]
        for _ in range(i + 1, tiles):
            row.append(message[at : at + LANES, :])
            at += LANES
        rows.append(jnp.concatenate(row, 1))
    both = jnp.concatenate(rows, 0)
    rid, cid = places(n)
    return jnp.where(cid >= rid, both, 0.0), jnp.where(cid < rid, both, 0.0)


def block_inverse(message, n):
    bond, x = unpacked(message, n)
    rid, cid = places(n)
    diagonal = rid == cid
    return jnp.where(diagonal, 1.0 / jnp.where(diagonal & (bond != 0.0), bond, 1.0), x)


def grown_inverse(message, x, size, stop):
    n = x.shape[-1]
    rid, cid = places(n)
    low_tri = unpacked(message, n)[0].T
    while size < stop:
        off = (rid // (2 * size) == cid // (2 * size)) & (rid // size > cid // size)
        part = split3(jnp.where(off, low_tri, 0.0))
        xs = split3(x)
        x = x - dot6(xs, split3(dot6(part, xs)))
        size *= 2
    return x


def upper_rows_kernel(sizes, packed, site, out):
    n = out.shape[-1]
    _, own, _ = own_sizes(sizes)
    x = split3(grown_inverse(packed[...], block_inverse(packed[...], n), PANEL, n))
    rid, cid = places(n)
    out[...] = dot6(split3(jnp.where((cid < own) & (rid < own), site[0, 0], 0.0)), x, 1)


def upper_rows(sizes, packed, site):
    n = site.shape[-1]
    return pl.pallas_call(
        upper_rows_kernel,
        out_shape=jax.ShapeDtypeStruct((n, n), f32),
        in_specs=[SM, VM, VM],
        out_specs=VM,
        compiler_params=params(16),
        name="upper_rows",
    )(sizes, packed, site)


SPLIT_AT = 4 * PANEL


def next_message(near, far):
    odd = lax.rem(lax.axis_index("row"), 2) == 1
    return jnp.where(jnp.broadcast_to(odd, near.shape), far[...], near[...])


def next_inverse_kernel(near, far, bond, applied, out, known):
    b, a = bond[...], time_step * applied[...]
    known[...] = lane_sums(((b, b), (b, a), (a, a)), 0)
    message = next_message(near, far)
    n = out.shape[-1]
    out[...] = grown_inverse(message, block_inverse(message, n), PANEL, SPLIT_AT)


def next_inverse(near, far, bond, applied):
    n = bond.shape[-1]
    return pl.pallas_call(
        next_inverse_kernel,
        out_shape=[jax.ShapeDtypeStruct((n, n), f32), jax.ShapeDtypeStruct((1, LANES), f32)],
        in_specs=[VM] * 4,
        out_specs=[VM] * 2,
        compiler_params=params(16),
        name="next_inverse",
    )(near, far, bond, applied)


def lower_rows_kernel(sizes, near, far, inv, site, top, out, low, sems):
    n = low.shape[-1]
    top_copy = pltpu.make_async_copy(top, out.at[0, 0], sems.at[0])
    top_copy.start()
    q, own, _ = own_sizes(sizes)
    count = lax.axis_size("row")
    after = sizes[jnp.minimum(q + 1, count - 1)]
    after = jnp.where(q + 1 < count, after, 0)
    x = split3(grown_inverse(next_message(near, far), inv[...], SPLIT_AT, n))
    rid, cid = places(n)
    low[...] = dot6(split3(jnp.where((cid < after) & (rid < own), site[0, 1], 0.0)), x, 1)
    low_copy = pltpu.make_async_copy(low, out.at[0, 1], sems.at[1])
    low_copy.start()
    top_copy.wait()
    low_copy.wait()


def lower_rows(sizes, near, far, inv, site, top):
    n = site.shape[-1]
    return pl.pallas_call(
        lower_rows_kernel,
        out_shape=jax.ShapeDtypeStruct((1, 2, n, n), f32),
        in_specs=[SM] + [VM] * 4 + [ANY],
        out_specs=ANY,
        scratch_shapes=[pltpu.VMEM((n, n), f32), pltpu.SemaphoreType.DMA((2,))],
        compiler_params=params(16),
        name="lower_rows",
    )(sizes, near, far, inv, site, top)


def channel(left, a, field, right):
    return dot3(split2(left[0, a]), split2(dot3(field, split2(right))))


def field_of(ref, n):
    return ref[...] if ref.shape[-1] == n else unpacked(ref[...], n)[0]


def moved_terms(field, left, right, base, total):
    f = split2(field)
    for a in range(right.shape[0]):
        total = total + channel(left, base + a, f, right[a])
    return total


def local_kernel(field, near, left, right, right_near, out):
    n = out.shape[-1]
    f = split2(field[...])
    total = jnp.zeros((n, n), f32)
    for a in range(W_DN + W_UP, left.shape[1]):
        total = total + channel(left, a, f, right[0, a])
    odd = lax.rem(lax.axis_index("row"), 2)
    out[...] = moved_terms(field_of(near, n), left, right_near, (1 - odd) * W_DN, total)


def local_terms(field, near, left, right, right_near):
    n = field.shape[-1]
    return pl.pallas_call(
        local_kernel,
        out_shape=jax.ShapeDtypeStruct((n, n), f32),
        in_specs=[VM] * 5,
        out_specs=VM,
        compiler_params=params(16),
        name="local_terms",
    )(field, near, left, right, right_near)


def with_far(mask, far, left, early, middle, late, part):
    n = part.shape[-1]
    q = lax.axis_index("row")
    kind = jnp.broadcast_to(far_kind(q) == 0, (n, n))
    half = early.shape[0]
    total = part[...]
    f = split2(field_of(far, n))
    for a in range(2 * half):
        pair = (early[a], middle[a]) if a < half else (middle[a - half], late[a - half])
        total = total + channel(left, lax.rem(q, 2) * W_DN + a, f, jnp.where(kind, *pair))
    return jnp.where(mask[...] > 0.0, total, 0.0)


def first_kernel(mask, far, left, early, middle, late, part, out):
    out[...] = with_far(mask, far, left, early, middle, late, part)


def first_apply(mask, far, left, right_far, part):
    n = part.shape[-1]
    return pl.pallas_call(
        first_kernel,
        out_shape=jax.ShapeDtypeStruct((n, n), f32),
        in_specs=[VM] * 7,
        out_specs=VM,
        compiler_params=params(16),
        name="first",
    )(mask, far, left, *right_far, part)


def lane_sums(pairs, first):
    lane = lax.broadcasted_iota(jnp.int32, (1, LANES), 1)
    row = jnp.zeros((1, LANES), f32)
    for i, (x, y) in enumerate(pairs):
        line = jnp.sum(jnp.sum(x * y, 0, keepdims=True), 1, keepdims=True)
        row = row + jnp.where(lane == first + i, line, 0.0)
    return row


def second_kernel(mask, far, left, early, middle, late, part, bond, applied, known, out, spread):
    twice = with_far(mask, far, left, early, middle, late, part)
    out[...] = twice
    b, a = bond[...], time_step * applied[...]
    t = (0.5 * time_step * time_step) * twice
    row = known[...] + lane_sums(((b, t), (a, t), (t, t)), 3)
    for i in range(spread.shape[0]):
        spread[i] = row


def second_apply(mask, far, left, right_far, part, bond, applied, known, count):
    n = part.shape[-1]
    return pl.pallas_call(
        second_kernel,
        out_shape=[
            jax.ShapeDtypeStruct((n, n), f32),
            pltpu.VMEM((count, 1, LANES), f32),
        ],
        in_specs=[VM] * 10,
        out_specs=[VM, VM],
        compiler_params=params(16),
        name="second",
    )(mask, far, left, *right_far, part, bond, applied, known)


def final_kernel(gathered, bond, applied, twice, out, staged, sems):
    sums = jnp.sum(gathered[...], 0)
    bb, ba, aa, bt, at, tt = (jnp.broadcast_to(sums[:, i : i + 1], (1, bond.shape[-1])) for i in range(6))
    rate = ba / bb
    c0 = 1.0 - rate + 0.5 * rate * rate
    c1 = 1.0 - rate
    norm = c0 * (c0 * bb + 2.0 * (c1 * ba + bt)) + c1 * (c1 * aa + 2.0 * at) + tt
    scale = jnp.sqrt(bb / norm)
    steps = (c0 * scale, (c1 * time_step) * scale, (0.5 * time_step * time_step) * scale)
    copies = []
    size = staged.shape[0] // CHUNKS
    for i in range(CHUNKS):
        part = pl.ds(i * size, size)
        staged[part, :] = steps[0] * bond[part, :] + steps[1] * applied[part, :] + steps[2] * twice[part, :]
        copies.append(pltpu.make_async_copy(staged.at[part], out.at[0, part], sems.at[i]))
        copies[i].start()
    for copy in copies:
        copy.wait()


def final(gathered, bond, applied, twice):
    n = bond.shape[-1]
    return pl.pallas_call(
        final_kernel,
        out_shape=jax.ShapeDtypeStruct((1, n, n), f32),
        in_specs=[VM] * 4,
        out_specs=ANY,
        scratch_shapes=[pltpu.VMEM((n, n), f32), pltpu.SemaphoreType.DMA((CHUNKS,))],
        compiler_params=params(4),
        name="final",
    )(gathered, bond, applied, twice)


def shifted_by(value, steps):
    count = lax.axis_size("row")
    first, last = max(0, -steps), min(count, count - steps)
    return lax.ppermute(value, "row", [(source, source + steps) for source in range(first, last)])


def swapped(value, first, step=2):
    count = lax.axis_size("row")
    pairs = [(i, i + 1) for i in range(first, count - 1, step)]
    return lax.ppermute(value, "row", pairs + [(j, i) for i, j in pairs])


def bond_update(site, left, right, sizes):
    count = lax.axis_size("row")
    source, early = take_early(site, right)
    early = swapped(early, 3, 4)
    lower = shifted_by(source, 1)
    middle, late, to_near = take_rest(right)
    middle = swapped(middle, 1)
    late = swapped(late, 1, 4)
    right_far = (early, middle, late)
    right_near = swapped(to_near, 0)
    bond, packed, mask = factor(sizes, site, lower)
    bond_far = swapped(packed, 1)
    bond_near = swapped(packed, 0)
    top = upper_rows(sizes, packed, site)
    part = local_terms(bond, bond_near, left, right, right_near)
    applied = first_apply(mask, bond_far, left, right_far, part)
    far = swapped(applied, 1)
    near = swapped(applied, 0)
    inv, known = next_inverse(bond_near, bond_far, bond, applied)
    part = local_terms(applied, near, left, right, right_near)
    twice, spread = second_apply(mask, far, left, right_far, part, bond, applied, known, count)
    gathered = lax.all_to_all(spread, "row", 0, 0, tiled=True)
    left_out = lower_rows(sizes, bond_near, bond_far, inv, site, top)
    bond_out = final(gathered, bond, applied, twice)
    return left_out, bond_out


def solution(mesh):
    placed = (
        P(("real", "row"), None, None, None),
        P(("real", "row"), None, None, None),
        P(("real", "row"), None, None, None),
        P("real"),
    )
    return jax.shard_map(
        bond_update,
        mesh=mesh,
        in_specs=placed,
        out_specs=(P(("real", "row"), None, None, None), P(("real", "row"), None, None)),
        check_vma=False,
    )
```

```python
import jax
import jax.numpy as jnp
from jax import lax
from jax.experimental import pallas as pl
from jax.experimental.pallas import tpu as pltpu
from jax.sharding import PartitionSpec as P

W_DN = 4
W_UP = 4
PANEL = 16
CHUNKS = 2
LANES = 128

f32, bf16 = jnp.float32, jnp.bfloat16
time_step = 0.15

VM = pl.BlockSpec(memory_space=pltpu.VMEM)
SM = pl.BlockSpec(memory_space=pltpu.SMEM)
ANY = pl.BlockSpec(memory_space=pl.ANY)
HB = pl.BlockSpec(memory_space=pltpu.HBM)


def params(mib):
    return pltpu.CompilerParams(vmem_limit_bytes=mib << 20)


def split2(x):
    hi = x.astype(bf16)
    return hi, (x - hi.astype(f32)).astype(bf16)


def split3(x):
    hi = x.astype(bf16)
    rest = x - hi.astype(f32)
    mid = rest.astype(bf16)
    return hi, mid, (rest - mid.astype(f32)).astype(bf16)


def dot(a, b, ca=1, cb=0):
    return lax.dot_general(a, b, (((ca,), (cb,)), ((), ())), preferred_element_type=f32)


def dot3(a, b):
    ah, al = a
    bh, bl = b
    return dot(ah, bh) + dot(al, bh) + dot(ah, bl)


def dot6(a, b, cb=0):
    ah, am, al = a
    bh, bm, bl = b
    pairs = ((ah, bh), (ah, bm), (am, bh), (am, bm), (ah, bl), (al, bh))
    return sum(dot(x, y, 1, cb) for x, y in pairs)


def places(n, rows=None):
    shape = (n if rows is None else rows, n)
    return lax.broadcasted_iota(jnp.int32, shape, 0), lax.broadcasted_iota(jnp.int32, shape, 1)


def own_sizes(sizes):
    q = lax.axis_index("row")
    return q, sizes[q], sizes[jnp.maximum(q - 1, 0)]


def far_kind(q):
    return lax.rem((q + 1) // 2, 2)


def first_far(q):
    return (1 - lax.rem(q, 2)) * W_DN


def run_copies(copies):
    for copy in copies:
        copy.start()
    for copy in copies:
        copy.wait()


def take_early_kernel(site, right, source, early, sems):
    half = early.shape[0]
    start = first_far(lax.axis_index("row"))
    run_copies(
        (
            pltpu.make_async_copy(site.at[0, 1], source, sems.at[0]),
            pltpu.make_async_copy(right.at[0, pl.ds(start, half)], early, sems.at[1]),
        )
    )


def take_rest_kernel(right, middle, late, near, sems):
    q = lax.axis_index("row")
    half = middle.shape[0]
    start = first_far(q)
    run_copies(
        (
            pltpu.make_async_copy(right.at[0, pl.ds(start + half, half)], middle, sems.at[0]),
            pltpu.make_async_copy(right.at[0, pl.ds(start, 2 * half)], late, sems.at[1]),
            pltpu.make_async_copy(right.at[0, pl.ds(lax.rem(q, 2) * W_DN, W_DN)], near, sems.at[2]),
        )
    )


def in_hbm(x):
    return pltpu.with_memory_space_constraint(x, pltpu.HBM)


def take_early(site, right):
    n = right.shape[-1]
    return pl.pallas_call(
        take_early_kernel,
        out_shape=[jax.ShapeDtypeStruct((n, n), f32), jax.ShapeDtypeStruct((W_UP // 2, n, n), f32)],
        in_specs=[HB] * 2,
        out_specs=[ANY] * 2,
        scratch_shapes=[pltpu.SemaphoreType.DMA((2,))],
        compiler_params=params(4),
        name="take_early",
    )(in_hbm(site), in_hbm(right))


def take_rest(right):
    n = right.shape[-1]
    return pl.pallas_call(
        take_rest_kernel,
        out_shape=[
            jax.ShapeDtypeStruct((W_UP // 2, n, n), f32),
            jax.ShapeDtypeStruct((W_UP, n, n), f32),
            jax.ShapeDtypeStruct((W_DN, n, n), f32),
        ],
        in_specs=[HB],
        out_specs=[ANY] * 3,
        scratch_shapes=[pltpu.SemaphoreType.DMA((3,))],
        compiler_params=params(4),
        name="take_rest",
    )(in_hbm(right))


def factor_kernel(sizes, site, lower, bond, packed, mask, inv0, work, turn, rows, erows, lstack, rstack):
    n = lower.shape[-1]
    _, own, prev = own_sizes(sizes)
    row_id, col_id = places(n)
    live_col = col_id < own
    top = jnp.where(live_col & (row_id < own), site[0, 0], 0.0)
    bot = jnp.where(live_col & (row_id < prev), lower[...], 0.0)
    mask[...] = jnp.where(live_col & (row_id < own), 1.0, 0.0)
    gram = jnp.where((row_id == col_id) & (row_id >= own), 1.0, 0.0)
    for part in (top, bot):
        gram = gram + dot6(split3(part.T), split3(part))
    work[pl.ds(0, n), :] = gram
    work[pl.ds(n, PANEL), :] = jnp.zeros((PANEL, n), f32)
    lstack[...] = jnp.zeros(lstack.shape, bf16)
    rstack[...] = jnp.zeros(rstack.shape, bf16)
    inv0[...] = jnp.zeros((n, n), f32)
    lane = lax.broadcasted_iota(jnp.int32, (PANEL, LANES), 1)
    sub = lax.broadcasted_iota(jnp.int32, (PANEL, LANES), 0)
    tiles = n // LANES

    def body(p, carry):
        r0 = pl.multiple_of(p * PANEL, PANEL)
        tile = pl.multiple_of((r0 // LANES) * LANES, LANES)
        off = r0 - tile
        after = r0 + PANEL
        ntile = pl.multiple_of(jnp.minimum((after // LANES) * LANES, n - LANES), LANES)
        noff = pl.multiple_of(lax.rem(after, LANES), PANEL)
        w = work[pl.ds(r0, PANEL), :]
        diag = work[pl.ds(r0, PANEL), pl.ds(tile, LANES)]
        turn[...] = work[pl.ds(r0, PANEL), pl.ds(ntile, LANES)].T
        update = dot(lstack[...], rstack[...], 0, 0)
        ahead = turn[pl.ds(noff, PANEL), :]
        here, there = [], []
        for j in range(PANEL):
            at = jnp.full((PANEL, LANES), off + j, jnp.int32)
            here.append(jnp.take_along_axis(diag, at, axis=1, mode="promise_in_bounds"))
            there.append(jnp.broadcast_to(ahead[:, j : j + 1], (PANEL, LANES)))
        ext = jnp.where(lane == off + sub, 1.0, 0.0)
        acc = jnp.zeros((PANEL, n), f32)
        for k in range(PANEL):
            scale = lax.rsqrt(jnp.broadcast_to(here[k][k : k + 1, :], (PANEL, LANES)))
            a = here[k] * scale
            b = there[k] * scale
            rk = w[k : k + 1, :] * jnp.concatenate([scale[:1]] * tiles, 1)
            ek = ext[k : k + 1, :] * scale[:1]
            rows[k : k + 1, :] = rk
            erows[k : k + 1, :] = ek
            spread = jnp.broadcast_to(rk, (PANEL, n))
            acc = acc + jnp.concatenate([b] * tiles, 1) * spread
            if k + 1 < PANEL:
                w = w - jnp.concatenate([a] * tiles, 1) * spread
                ext = ext - a * jnp.broadcast_to(ek, (PANEL, LANES))
            for j in range(k + 1, PANEL):
                s = jnp.broadcast_to(a[j : j + 1, :], (PANEL, LANES))
                here[j] = here[j] - a * s
                there[j] = there[j] - b * s
        work[pl.ds(0, n), :] = work[pl.ds(0, n), :] - update
        work[pl.ds(after, PANEL), :] = work[pl.ds(after, PANEL), :] - acc
        r = rows[...]
        inv0[pl.ds(r0, PANEL), pl.ds(tile, LANES)] = erows[...]
        h, m, l = split3(r)
        for i, (x, y) in enumerate(((h, h), (m, h), (h, m), (m, m), (l, h), (h, l))):
            lstack[pl.ds(i * PANEL, PANEL), :] = x
            rstack[pl.ds(i * PANEL, PANEL), :] = y
        rid, cid = places(n, PANEL)
        rid = rid + r0
        bond[pl.ds(r0, PANEL), :] = jnp.where((cid >= rid) & (rid < own) & (cid < own), r, 0.0)
        return carry

    lax.fori_loop(0, n // PANEL, body, 0)
    rid, cid = places(LANES)
    diagonal = []
    for i in range(tiles):
        where = (pl.ds(i * LANES, LANES), pl.ds(i * LANES, LANES))
        diagonal.append(jnp.where(rid > cid, inv0[where], bond[where]))
    at = 0
    for part in fold(diagonal):
        packed[pl.ds(at, part.shape[0]), :] = part
        at += part.shape[0]
    for i in range(tiles):
        for j in range(i + 1, tiles):
            packed[pl.ds(at, LANES), :] = bond[pl.ds(i * LANES, LANES), pl.ds(j * LANES, LANES)]
            at += LANES


def fold(diagonal):
    half = LANES // 2
    low = lax.broadcasted_iota(jnp.int32, (half, LANES), 1) < half
    parts = []
    for i in range(0, len(diagonal) - 1, 2):
        first, second = diagonal[i], diagonal[i + 1]
        parts.append(first[:half])
        parts.append(jnp.where(low, pltpu.roll(second[:half], half, 1), first[half:]))
        parts.append(jnp.where(low, second[:half], second[half:]))
    return parts + diagonal[len(diagonal) - len(diagonal) % 2 :]


def unfold(message, tiles):
    half = LANES // 2
    low = lax.broadcasted_iota(jnp.int32, (half, LANES), 1) < half
    diagonal, at = [], 0
    for _ in range(0, tiles - 1, 2):
        a, b, c = (message[at + i * half : at + (i + 1) * half, :] for i in range(3))
        diagonal.append(jnp.concatenate([a, jnp.where(low, 0.0, b)], 0))
        diagonal.append(jnp.concatenate([jnp.where(low, c, pltpu.roll(b, half, 1)), jnp.where(low, 0.0, c)], 0))
        at += 3 * half
    if tiles % 2:
        diagonal.append(message[at : at + LANES, :])
        at += LANES
    return diagonal, at


def factor(sizes, site, lower):
    n = lower.shape[-1]
    tiles = n // LANES
    return pl.pallas_call(
        factor_kernel,
        out_shape=[
            jax.ShapeDtypeStruct((n, n), f32),
            jax.ShapeDtypeStruct((tiles * (tiles + 1) // 2 * LANES - tiles // 2 * (LANES // 2), LANES), f32),
            jax.ShapeDtypeStruct((n, n), f32),
        ],
        in_specs=[SM, VM, VM],
        out_specs=[VM] * 3,
        scratch_shapes=[
            pltpu.VMEM((n, n), f32),
            pltpu.VMEM((n + PANEL, n), f32),
            pltpu.VMEM((LANES, PANEL), f32),
            pltpu.VMEM((PANEL, n), f32),
            pltpu.VMEM((PANEL, LANES), f32),
            pltpu.VMEM((6 * PANEL, n), bf16),
            pltpu.VMEM((6 * PANEL, n), bf16),
        ],
        compiler_params=params(12),
        name="factor",
    )(sizes, site, lower)


def unpacked(message, n):
    tiles = n // LANES
    diagonal, at = unfold(message, tiles)
    rows = []
    for i in range(tiles):
        row = [jnp.zeros((LANES, LANES), f32)] * i + [diagonal[i]]
        for _ in range(i + 1, tiles):
            row.append(message[at : at + LANES, :])
            at += LANES
        rows.append(jnp.concatenate(row, 1))
    both = jnp.concatenate(rows, 0)
    rid, cid = places(n)
    return jnp.where(cid >= rid, both, 0.0), jnp.where(cid < rid, both, 0.0)


def block_inverse(message, n):
    bond, x = unpacked(message, n)
    rid, cid = places(n)
    diagonal = rid == cid
    return jnp.where(diagonal, 1.0 / jnp.where(diagonal & (bond != 0.0), bond, 1.0), x)


def grown_inverse(message, x, size, stop):
    n = x.shape[-1]
    rid, cid = places(n)
    low_tri = unpacked(message, n)[0].T
    while size < stop:
        off = (rid // (2 * size) == cid // (2 * size)) & (rid // size > cid // size)
        part = split3(jnp.where(off, low_tri, 0.0))
        xs = split3(x)
        x = x - dot6(xs, split3(dot6(part, xs)))
        size *= 2
    return x


def upper_rows_kernel(sizes, packed, site, out):
    n = out.shape[-1]
    _, own, _ = own_sizes(sizes)
    x = split3(grown_inverse(packed[...], block_inverse(packed[...], n), PANEL, n))
    rid, cid = places(n)
    out[...] = dot6(split3(jnp.where((cid < own) & (rid < own), site[0, 0], 0.0)), x, 1)


def upper_rows(sizes, packed, site):
    n = site.shape[-1]
    return pl.pallas_call(
        upper_rows_kernel,
        out_shape=jax.ShapeDtypeStruct((n, n), f32),
        in_specs=[SM, VM, VM],
        out_specs=VM,
        compiler_params=params(16),
        name="upper_rows",
    )(sizes, packed, site)


SPLIT_AT = 4 * PANEL


def next_message(near, far):
    odd = lax.rem(lax.axis_index("row"), 2) == 1
    return jnp.where(jnp.broadcast_to(odd, near.shape), far[...], near[...])


def next_inverse_kernel(near, far, bond, applied, out, known):
    b, a = bond[...], time_step * applied[...]
    known[...] = lane_sums(((b, b), (b, a), (a, a)), 0)
    message = next_message(near, far)
    n = out.shape[-1]
    out[...] = grown_inverse(message, block_inverse(message, n), PANEL, SPLIT_AT)


def next_inverse(near, far, bond, applied):
    n = bond.shape[-1]
    return pl.pallas_call(
        next_inverse_kernel,
        out_shape=[jax.ShapeDtypeStruct((n, n), f32), jax.ShapeDtypeStruct((1, LANES), f32)],
        in_specs=[VM] * 4,
        out_specs=[VM] * 2,
        compiler_params=params(16),
        name="next_inverse",
    )(near, far, bond, applied)


def lower_rows_kernel(sizes, near, far, inv, site, top, out, low, sems):
    n = low.shape[-1]
    top_copy = pltpu.make_async_copy(top, out.at[0, 0], sems.at[0])
    top_copy.start()
    q, own, _ = own_sizes(sizes)
    count = lax.axis_size("row")
    after = sizes[jnp.minimum(q + 1, count - 1)]
    after = jnp.where(q + 1 < count, after, 0)
    x = split3(grown_inverse(next_message(near, far), inv[...], SPLIT_AT, n))
    rid, cid = places(n)
    low[...] = dot6(split3(jnp.where((cid < after) & (rid < own), site[0, 1], 0.0)), x, 1)
    low_copy = pltpu.make_async_copy(low, out.at[0, 1], sems.at[1])
    low_copy.start()
    top_copy.wait()
    low_copy.wait()


def lower_rows(sizes, near, far, inv, site, top):
    n = site.shape[-1]
    return pl.pallas_call(
        lower_rows_kernel,
        out_shape=jax.ShapeDtypeStruct((1, 2, n, n), f32),
        in_specs=[SM] + [VM] * 4 + [ANY],
        out_specs=ANY,
        scratch_shapes=[pltpu.VMEM((n, n), f32), pltpu.SemaphoreType.DMA((2,))],
        compiler_params=params(16),
        name="lower_rows",
    )(sizes, near, far, inv, site, top)


def channel(left, a, field, right):
    return dot3(split2(left[0, a]), split2(dot3(field, split2(right))))


def field_of(ref, n):
    return ref[...] if ref.shape[-1] == n else unpacked(ref[...], n)[0]


def moved_terms(field, left, right, base, total):
    f = split2(field)
    for a in range(right.shape[0]):
        total = total + channel(left, base + a, f, right[a])
    return total


def local_kernel(field, near, left, right, right_near, out):
    n = out.shape[-1]
    f = split2(field[...])
    total = jnp.zeros((n, n), f32)
    for a in range(W_DN + W_UP, left.shape[1]):
        total = total + channel(left, a, f, right[0, a])
    odd = lax.rem(lax.axis_index("row"), 2)
    out[...] = moved_terms(field_of(near, n), left, right_near, (1 - odd) * W_DN, total)


def local_terms(field, near, left, right, right_near):
    n = field.shape[-1]
    return pl.pallas_call(
        local_kernel,
        out_shape=jax.ShapeDtypeStruct((n, n), f32),
        in_specs=[VM] * 5,
        out_specs=VM,
        compiler_params=params(16),
        name="local_terms",
    )(field, near, left, right, right_near)


def with_far(mask, far, left, early, middle, late, part):
    n = part.shape[-1]
    q = lax.axis_index("row")
    kind = jnp.broadcast_to(far_kind(q) == 0, (n, n))
    half = early.shape[0]
    total = part[...]
    f = split2(field_of(far, n))
    for a in range(2 * half):
        of_kind = early[a] if a < half else middle[a - half]
        total = total + channel(left, lax.rem(q, 2) * W_DN + a, f, jnp.where(kind, of_kind, late[a]))
    return jnp.where(mask[...] > 0.0, total, 0.0)


def first_kernel(mask, far, left, early, middle, late, part, out):
    out[...] = with_far(mask, far, left, early, middle, late, part)


def first_apply(mask, far, left, right_far, part):
    n = part.shape[-1]
    return pl.pallas_call(
        first_kernel,
        out_shape=jax.ShapeDtypeStruct((n, n), f32),
        in_specs=[VM] * 7,
        out_specs=VM,
        compiler_params=params(16),
        name="first",
    )(mask, far, left, *right_far, part)


def lane_sums(pairs, first):
    lane = lax.broadcasted_iota(jnp.int32, (1, LANES), 1)
    row = jnp.zeros((1, LANES), f32)
    for i, (x, y) in enumerate(pairs):
        line = jnp.sum(jnp.sum(x * y, 0, keepdims=True), 1, keepdims=True)
        row = row + jnp.where(lane == first + i, line, 0.0)
    return row


def second_kernel(mask, far, left, early, middle, late, part, bond, applied, known, out, spread):
    twice = with_far(mask, far, left, early, middle, late, part)
    out[...] = twice
    b, a = bond[...], time_step * applied[...]
    t = (0.5 * time_step * time_step) * twice
    row = known[...] + lane_sums(((b, t), (a, t), (t, t)), 3)
    for i in range(spread.shape[0]):
        spread[i] = row


def second_apply(mask, far, left, right_far, part, bond, applied, known, count):
    n = part.shape[-1]
    return pl.pallas_call(
        second_kernel,
        out_shape=[
            jax.ShapeDtypeStruct((n, n), f32),
            pltpu.VMEM((count, 1, LANES), f32),
        ],
        in_specs=[VM] * 10,
        out_specs=[VM, VM],
        compiler_params=params(16),
        name="second",
    )(mask, far, left, *right_far, part, bond, applied, known)


def final_kernel(gathered, bond, applied, twice, out, staged, sems):
    sums = jnp.sum(gathered[...], 0)
    bb, ba, aa, bt, at, tt = (jnp.broadcast_to(sums[:, i : i + 1], (1, bond.shape[-1])) for i in range(6))
    rate = ba / bb
    c0 = 1.0 - rate + 0.5 * rate * rate
    c1 = 1.0 - rate
    norm = c0 * (c0 * bb + 2.0 * (c1 * ba + bt)) + c1 * (c1 * aa + 2.0 * at) + tt
    scale = jnp.sqrt(bb / norm)
    steps = (c0 * scale, (c1 * time_step) * scale, (0.5 * time_step * time_step) * scale)
    copies = []
    size = staged.shape[0] // CHUNKS
    for i in range(CHUNKS):
        part = pl.ds(i * size, size)
        staged[part, :] = steps[0] * bond[part, :] + steps[1] * applied[part, :] + steps[2] * twice[part, :]
        copies.append(pltpu.make_async_copy(staged.at[part], out.at[0, part], sems.at[i]))
        copies[i].start()
    for copy in copies:
        copy.wait()


def final(gathered, bond, applied, twice):
    n = bond.shape[-1]
    return pl.pallas_call(
        final_kernel,
        out_shape=jax.ShapeDtypeStruct((1, n, n), f32),
        in_specs=[VM] * 4,
        out_specs=ANY,
        scratch_shapes=[pltpu.VMEM((n, n), f32), pltpu.SemaphoreType.DMA((CHUNKS,))],
        compiler_params=params(4),
        name="final",
    )(gathered, bond, applied, twice)


def shifted_by(value, steps):
    count = lax.axis_size("row")
    first, last = max(0, -steps), min(count, count - steps)
    return lax.ppermute(value, "row", [(source, source + steps) for source in range(first, last)])


def swapped(value, first, step=2):
    count = lax.axis_size("row")
    pairs = [(i, i + 1) for i in range(first, count - 1, step)]
    return lax.ppermute(value, "row", pairs + [(j, i) for i, j in pairs])


def bond_update(site, left, right, sizes):
    count = lax.axis_size("row")
    source, early = take_early(site, right)
    early = swapped(early, 3, 4)
    lower = shifted_by(source, 1)
    middle, late, to_near = take_rest(right)
    middle = swapped(middle, 3, 4)
    late = swapped(late, 1, 4)
    right_far = (early, middle, late)
    right_near = swapped(to_near, 0)
    bond, packed, mask = factor(sizes, site, lower)
    bond_far = swapped(packed, 1)
    bond_near = swapped(packed, 0)
    top = upper_rows(sizes, packed, site)
    part = local_terms(bond, bond_near, left, right, right_near)
    applied = first_apply(mask, bond_far, left, right_far, part)
    far = swapped(applied, 1)
    near = swapped(applied, 0)
    inv, known = next_inverse(bond_near, bond_far, bond, applied)
    part = local_terms(applied, near, left, right, right_near)
    twice, spread = second_apply(mask, far, left, right_far, part, bond, applied, known, count)
    gathered = lax.all_to_all(spread, "row", 0, 0, tiled=True)
    left_out = lower_rows(sizes, bond_near, bond_far, inv, site, top)
    bond_out = final(gathered, bond, applied, twice)
    return left_out, bond_out


def solution(mesh):
    placed = (
        P(("real", "row"), None, None, None),
        P(("real", "row"), None, None, None),
        P(("real", "row"), None, None, None),
        P("real"),
    )
    return jax.shard_map(
        bond_update,
        mesh=mesh,
        in_specs=placed,
        out_specs=(P(("real", "row"), None, None, None), P(("real", "row"), None, None)),
        check_vma=False,
    )
```
